32 devices in a mesh: dp: 8 (over z, y), tensor: 4 (over x, core).
Axes of the slice: x: 2, y: 2, z: 4, core: 2. Of those that a mesh axis runs over, the one named last changes fastest.
Arguments:
- qkv: bfloat16 [3, 2048, 4096], P(None, 'dp', 'tensor'), may hold values from -6 to 6
- segment_ids: int32 [8, 4, 64], P('dp'), may hold values from 0 to 1, never falling along the last dimension, each value on 1 to 63 neighbouring positions
- out_weight: bfloat16 [4096, 4096], P(None, 'tensor'), may hold values from -0.09375 to 0.09375
- out_bias: bfloat16 [4096], replicated, may hold values from -3 to 3
- upstream: bfloat16 [2048, 4096], P(('dp', 'tensor')), may hold values from -6 to 6
- pre_act: bfloat16 [2048, 8192], P('dp', 'tensor'), may hold values from -6 to 6
- down_weight: bfloat16 [4096, 8192], P('dp', 'tensor'), may hold values from -0.0625 to 0.0625
Outputs:
- attention_out: float32 [2048, 4096], P(('dp', 'tensor'))
- act_grad: float32 [2048, 8192], P('dp', 'tensor')
- weight_grad: float32 [4096, 8192], P('dp', 'tensor')
The draws below stay inside these ranges and needn't reach their ends.
Inputs may be any that keep to these rules, and one draw needn't show every extreme that they name: `segment_ids`: within each pack the ids never fall; 2 images a pack, each of 1 to 63 tokens.
All inputs are finite; a program needn't handle non-finite values.
Results may differ from the reference program's by a relative error of at most 0.0055.
Values may be sent and summed in bfloat16 or wider, within the bound.
A program may use at most 128 MiB of HBM per device.

```python
import math
import jax
import jax.numpy as jnp
import numpy as np
from jax import lax

D = 4096
HEADS = 32
HEAD = 128
FF = 8192
ROWS_DEV = 64
TOKENS = 256
BATCH = 2048
HD = 4096
IMG_PACK = 2
MOST_IMG = 63
N_DP = 8
N_TENSOR = 4


def draw_qkv(key, part):
    sample = jax.random.truncated_normal(key, -6.0, 6.0, (3, BATCH, HD), jnp.float32)
    return sample.astype(jnp.bfloat16)


def spiked(result, key, source, target, shards_of, factor):
    def block_of(dim):
        return (jnp.arange(result.shape[dim]) // (result.shape[dim] // shards_of)).reshape((-1,) + (1,) * (result.ndim - 1 - dim))

    near = jax.random.permutation(key, shards_of)[block_of(target)]
    far = (block_of(target) + shards_of // 2) % shards_of
    return jnp.where((block_of(source) == near) | (block_of(source) == far), factor * result, result)


def shard_levels(stream_key, extent, pieces, least, largest):
    loudness = 1.0
    for dim, parts in pieces:
        steps = jax.random.uniform(jax.random.fold_in(jax.random.fold_in(stream_key, 6), dim), (parts,), jnp.float32, least / len(pieces), largest / len(pieces))
        loudness = loudness * jnp.repeat(jnp.exp(steps), extent[dim] // parts).reshape((-1,) + (1,) * (len(extent) - 1 - dim))
    return loudness


def profile(number_of, total, limit, lean):
    weights = [(1 << 20) // math.isqrt(rank ** lean) + 1 for rank in range(2, number_of + 1)]
    surplus, given = total - limit - (number_of - 1), [1] * (number_of - 1)
    while surplus > 0:
        movable = [i for i in range(number_of - 1) if given[i] < limit]
        mass, remaining = sum([weights[i] for i in movable]), surplus
        for i in movable:
            addition = min(limit - given[i], max(1, remaining * weights[i] // mass), surplus)
            given[i] = given[i] + addition
            surplus = surplus - addition
    return np.array([limit] + given)


def uneven(stream_key, number_of, total, most, lean):
    if number_of == 2:
        one = jax.random.randint(stream_key, (), max(1, total - most), min(most, total - 1) + 1)
        return jnp.stack([one, total - one])
    lengths = jnp.asarray(profile(number_of, total, most, lean), jnp.int32)
    pairs = (number_of - 1) // 2
    donor, receiver = lengths[1:1 + 2 * pairs:2], lengths[2:2 + 2 * pairs:2]
    slack = jnp.minimum(donor - 1, most - receiver)
    passed = jax.random.randint(jax.random.fold_in(stream_key, 1), (pairs,), 0, 1 << 20) % (slack + 1)
    lengths = lengths.at[1:1 + 2 * pairs:2].set(donor - passed).at[2:2 + 2 * pairs:2].set(receiver + passed)
    return lengths[jax.random.permutation(jax.random.fold_in(stream_key, 2), number_of)]


def normal_values(own_key, dims, deviation, most, shards=(), kind=jnp.bfloat16):
    result = deviation * jax.random.normal(own_key, dims, jnp.float32)
    if shards:
        result = result * shard_levels(own_key, dims, shards, -0.22, 0.18)
    return jnp.clip(result, -most, most).astype(kind)


def noise_with(key, extent, spread, most, shards, heavy, kind=jnp.bfloat16):
    values = spread * jax.random.normal(key, extent, jnp.float32)
    if shards:
        values = values * shard_levels(key, extent, shards, -0.22, 0.18)
    return jnp.clip(spiked(values, jax.random.fold_in(key, 3), *heavy), -most, most).astype(kind)


def setup_inputs(seed: int = 0) -> dict:
    splits = jax.random.split(jax.random.key(seed), 8)
    return {
        "qkv": draw_qkv(jax.random.fold_in(splits[7], 71), 0),
        "segment_ids": jax.vmap(lambda own: jnp.searchsorted(jnp.cumsum(uneven(own, IMG_PACK, ROWS_DEV, MOST_IMG, 2)), jnp.arange(ROWS_DEV), side="right"))(jax.random.split(splits[1], N_DP * N_TENSOR)).reshape((N_DP, N_TENSOR, ROWS_DEV)).astype(jnp.int32),
        "out_weight": normal_values(splits[2], (D, HD), HD ** -0.5, 0.09375, ((1, 4),)),
        "out_bias": normal_values(splits[3], (D,), 0.5, 3.0),
        "upstream": noise_with(splits[4], (BATCH, D), 1.0, 6.0, ((0, 32),), (0, 1, 32, 2.75)),
        "pre_act": normal_values(splits[5], (BATCH, FF), 1.0, 6.0, ((0, 8), (1, 4))),
        "down_weight": normal_values(splits[6], (D, FF), FF ** -0.5, 0.0625, ((0, 8), (1, 4))),
    }


root_half = 1.0 / math.sqrt(2.0)
inv_root_tau = 1.0 / math.sqrt(2.0 * math.pi)

def gelu_exact(argument):
    return 0.5 * argument * (1.0 + lax.erf(argument * root_half))

def gelu_slope(argument):
    return 0.5 * (1.0 + lax.erf(argument * root_half)) + argument * jnp.exp(-0.5 * argument * argument) * inv_root_tau

def attend(bundle):
    queries, key_rows, value_rows, labels = bundle
    length = queries.shape[0]
    queries = queries.reshape(length, HEADS, HEAD).astype(jnp.float32)
    key_rows = key_rows.reshape(length, HEADS, HEAD).astype(jnp.float32)
    value_rows = value_rows.reshape(length, HEADS, HEAD).astype(jnp.float32)
    scores = jnp.einsum('qhd,khd->hqk', queries, key_rows) * (1.0 / math.sqrt(HEAD))
    pack_of = jnp.arange(length, dtype=jnp.int32) // ROWS_DEV
    same_image = ((labels[:, None] == labels[None, :]) & (pack_of[:, None] == pack_of[None, :]))[None]
    masked = jnp.where(same_image, scores, -1e+30)
    row_top = lax.optimization_barrier(jnp.max(masked, axis=2, keepdims=True))
    exponent = jnp.where(same_image, jnp.exp(masked - row_top), 0.0)
    weights = (exponent / lax.optimization_barrier(jnp.sum(exponent, axis=2, keepdims=True))).astype(jnp.bfloat16)
    context = jnp.einsum('hqk,khd->qhd', weights.astype(jnp.float32), value_rows)
    return context.reshape(length, HD).astype(jnp.bfloat16)

def reference(qkv, segment_ids, out_weight, out_bias, upstream, pre_act, down_weight):
    packed = qkv.reshape(3, N_DP, TOKENS, HD)
    labels = segment_ids.reshape(N_DP, TOKENS)
    context = lax.map(attend, (packed[0], packed[1], packed[2], labels))
    context = context.reshape(BATCH, HD)
    share = HD // N_TENSOR
    running = jnp.zeros((BATCH, D), jnp.float32)
    for member in range(N_TENSOR):
        ctx_part = context[:, member * share:(member + 1) * share]
        weight_part = out_weight[:, member * share:(member + 1) * share]
        partial_value = lax.dot_general(ctx_part, weight_part, (((1,), (1,)), ((), ())), preferred_element_type=jnp.float32)
        rounded = lax.optimization_barrier(partial_value.astype(jnp.bfloat16))
        running = running + rounded.astype(jnp.float32)
    attention_out = running + out_bias.astype(jnp.float32)
    hidden_grad = jnp.dot(upstream, down_weight, preferred_element_type=jnp.float32)
    preact = pre_act.astype(jnp.float32)
    act_grad = hidden_grad * gelu_slope(preact)
    activation = gelu_exact(preact).astype(jnp.bfloat16)
    weight_grad = lax.dot_general(upstream, activation, (((0,), (0,)), ((), ())), preferred_element_type=jnp.float32) / N_DP
    return (attention_out, act_grad, weight_grad)
```

```python
import functools
import math

import jax
import jax.numpy as jnp
from jax import lax
from jax.experimental import pallas as pl
from jax.experimental.pallas import tpu as pltpu
from jax.sharding import PartitionSpec as P

HEAD = 128
ROWS_DEV = 64
CHUNKS = 8
LAG = 3
AHEAD = 6
EARLY = 2
HEADS_TICK = 2
SPANS_TICK = 2
PIECES = 4

root_half = 1.0 / math.sqrt(2.0)
inv_root_tau = 1.0 / math.sqrt(2.0 * math.pi)


def gelu_exact(argument):
    return 0.5 * argument * (1.0 + lax.erf(argument * root_half))


def gelu_slope(argument):
    return (
        0.5 * (1.0 + lax.erf(argument * root_half))
        + argument * jnp.exp(-0.5 * argument * argument) * inv_root_tau
    )


def kernel(
    sizes,
    qkv_hbm, segments, ow_hbm, bias, up_hbm, pre, w_hbm,
    att_out, hid_out, wg_out,
    qkv, ow, ctx, part, att_recv,
    u_all, u_t, w_all, a_all, a_own, same_ref, h_right, h_left, g_send, g_recv,
    local_sem, loc_wa, att_s, att_r,
    uz_s, uz_r, ux_s, ux_r, uc_s, uc_r,
    w_s, w_r, ar_s, ar_r, al_s, al_r,
    hr_s, hr_r, hl_s, hl_r, g_s, g_r,
):
    OUT, INN, TEN = sizes
    XS = TEN // 2
    g = lax.axis_index("dp")
    t = lax.axis_index("tensor")
    o, i = g // INN, lax.rem(g, INN)
    x, core = t // 2, lax.rem(t, 2)
    rows_w, ff = w_hbm.shape
    rows = up_hbm.shape[0]
    tokens = rows * TEN
    fc = ff // CHUNKS
    dcols = rows_w * INN
    HOPS = OUT - 1

    def remote(src, dst, ssem, rsem, dp, tensor):
        return pltpu.make_async_remote_copy(
            src_ref=src, dst_ref=dst, send_sem=ssem, recv_sem=rsem,
            device_id={"dp": dp, "tensor": tensor},
            device_id_type=pl.DeviceIdType.MESH,
        )

    def cols(c):
        return pl.ds(pl.multiple_of(c * fc, fc), fc)

    def u_rows(oo, tt):
        return u_all.at[pl.ds(pl.multiple_of((oo * TEN + tt) * rows, rows), rows), :]

    def a_rows(c, oo):
        return a_all.at[c, pl.ds(pl.multiple_of(oo * tokens, tokens), tokens), :]

    def w_rows(c, ii):
        return w_all.at[c, pl.ds(pl.multiple_of(ii * rows_w, rows_w), rows_w), :]

    def uz(j):
        to = lax.rem(o + j, OUT)
        return remote(
            up_hbm.at[:, pl.ds(pl.multiple_of(to * dcols, dcols), dcols)],
            u_rows(o, t), uz_s.at[j - 1], uz_r.at[j - 1], to * INN + i, t,
        )

    def ux(j, k):
        block = u_rows(lax.rem(o - j + OUT, OUT), t)
        return remote(block, block, ux_s.at[j, k - 1], ux_r.at[j, k - 1], g,
                      lax.rem(x + k, XS) * 2 + core)

    def uc(j, k):
        block = u_rows(lax.rem(o - j + OUT, OUT), lax.rem(x - k + XS, XS) * 2 + core)
        return remote(block, block, uc_s.at[j, k], uc_r.at[j, k], g, x * 2 + 1 - core)

    def wx(c, j):
        return remote(w_hbm.at[:, cols(c)], w_rows(c, i), w_s.at[c, j - 1], w_r.at[c, j - 1],
                      o * INN + lax.rem(i + j, INN), t)

    def a_right(c, s, own):
        dst = a_rows(c, jnp.maximum(o - s, 0))
        src = a_own.at[c] if own else dst
        return remote(src, dst, ar_s.at[c, s], ar_r.at[c, s],
                      jnp.minimum(o + 1, OUT - 1) * INN + i, t)

    def a_left(c, s, own):
        dst = a_rows(c, jnp.minimum(o + s, OUT - 1))
        src = a_own.at[c] if own else dst
        return remote(src, dst, al_s.at[c, s], al_r.at[c, s],
                      jnp.maximum(o - 1, 0) * INN + i, t)

    def h_r(c, e):
        return remote(h_right.at[c, e], h_right.at[c, e], hr_s.at[c, e], hr_r.at[c, e],
                      jnp.minimum(o + 1, OUT - 1) * INN + i, t)

    def h_l(c, e):
        return remote(h_left.at[c, e], h_left.at[c, e], hl_s.at[c, e], hl_r.at[c, e],
                      jnp.maximum(o - 1, 0) * INN + i, t)

    def gx(c, j):
        return remote(g_send.at[c, j - 1], g_recv.at[c, j - 1], g_s.at[c, j - 1], g_r.at[c, j - 1],
                      o * INN + lax.rem(i + j, INN), t)

    def att(j):
        to = lax.rem(t + j, TEN)
        return remote(part.at[pl.ds(pl.multiple_of(to * rows, rows), rows), :],
                      att_recv.at[j - 1], att_s.at[j - 1], att_r.at[j - 1], g, to)

    def own_w(c):
        return pltpu.make_async_copy(w_hbm.at[:, cols(c)], w_rows(c, i), loc_wa.at[0, c])

    def loop(count, fn):
        def step(index, carry):
            fn(index)
            return carry
        lax.fori_loop(0, count, step, 0)

    own_u = pltpu.make_async_copy(
        up_hbm.at[:, pl.ds(pl.multiple_of(o * dcols, dcols), dcols)], u_rows(o, t), local_sem.at[0])
    load_qkv = pltpu.make_async_copy(qkv_hbm, qkv, local_sem.at[1])
    load_ow = pltpu.make_async_copy(ow_hbm, ow, local_sem.at[2])

    own_u.start()
    for j in range(1, OUT):
        uz(j).start()
    load_qkv.start()

    def a_tick(k):
        for s in range(OUT):
            n = k - s * LAG
            if isinstance(k, int):
                if n >= 0 and n % HOPS == 0 and n // HOPS < CHUNKS:
                    a_step(n // HOPS, s)
            else:
                @pl.when((n >= 0) & (lax.rem(n, HOPS) == 0) & (n < CHUNKS * HOPS))
                def _():
                    a_step(n // HOPS, s)

    def a_step(c, s):
        @pl.when(o >= s)
        def _():
            if s:
                got = a_rows(c, o - s)
                remote(got, got, ar_s.at[c, s - 1], ar_r.at[c, s - 1], g, t).wait_recv()
            if s < HOPS:
                @pl.when(o < OUT - 1)
                def _():
                    a_right(c, s, s == 0).start()

        @pl.when(o + s <= OUT - 1)
        def _():
            if s:
                got = a_rows(c, o + s)
                remote(got, got, al_s.at[c, s - 1], al_r.at[c, s - 1], g, t).wait_recv()
            if s < HOPS:
                @pl.when(o > 0)
                def _():
                    a_left(c, s, s == 0).start()

    def start_w(c):
        for j in range(1, INN):
            wx(c, j).start()
        own_w(c).start()

    loop(CHUNKS, start_w)
    load_ow.start()

    def activate(c):
        act = gelu_exact(pre[:, cols(c)].astype(jnp.float32)).astype(jnp.bfloat16)
        a_own[c] = act
        a_all[c, pl.ds(pl.multiple_of(o * tokens, tokens), tokens), :] = act

    loop(min(EARLY, CHUNKS), activate)
    for k in range(AHEAD):
        a_tick(k)
    own_u.wait()
    for k in range(1, XS):
        ux(0, k).start()
    uc(0, 0).start()

    for j in range(1, OUT):
        uz(j).wait_recv()
        for k in range(1, XS):
            ux(j, k).start()
        uc(j, 0).start()
    loop(CHUNKS - min(EARLY, CHUNKS), lambda c: activate(c + EARLY))
    load_qkv.wait()
    load_ow.wait()
    for j in range(OUT):
        for k in range(1, XS):
            ux(j, k).wait_recv()
            uc(j, k).start()
    for j in range(OUT):
        for k in range(XS):
            uc(j, k).wait_recv()

    heads = qkv.shape[2] // HEAD
    block = min(tokens, 4 * ROWS_DEV)
    scale = 1.0 / math.sqrt(HEAD)

    labels = segments[0].astype(jnp.float32)
    packs, length = labels.shape
    spread = (
        lax.rem(lax.broadcasted_iota(jnp.int32, (length, tokens), 1), length)
        == lax.broadcasted_iota(jnp.int32, (length, tokens), 0)
    ).astype(jnp.float32)
    wide = jnp.dot(labels, spread, preferred_element_type=jnp.float32)
    pack = lax.broadcasted_iota(jnp.int32, (packs, tokens), 0)
    here = lax.broadcasted_iota(jnp.int32, (packs, tokens), 1) // length == pack
    name = jnp.sum(
        jnp.where(here, wide + 2.0 * pack.astype(jnp.float32), 0.0), axis=0, keepdims=True)
    for b in range(tokens // block):
        across = jnp.broadcast_to(name[:, b * block : (b + 1) * block], (block, block))
        same_ref[b] = (across == across.T).astype(jnp.float32)

    def head(h):
        lanes = pl.ds(pl.multiple_of(h * HEAD, HEAD), HEAD)
        for b in range(tokens // block):
            mine = slice(b * block, (b + 1) * block)
            same = same_ref[b] > 0.5
            scores = lax.dot_general(
                qkv[0, mine, lanes], qkv[1, mine, lanes], (((1,), (1,)), ((), ())),
                preferred_element_type=jnp.float32) * scale
            masked = jnp.where(same, scores, -1e30)
            top = jnp.max(masked, axis=1, keepdims=True)
            exponent = jnp.where(same, jnp.exp(masked - top), 0.0)
            weights = (exponent / jnp.sum(exponent, axis=1, keepdims=True)).astype(jnp.bfloat16)
            ctx[mine, lanes] = jnp.dot(
                weights, qkv[2, mine, lanes], preferred_element_type=jnp.float32
            ).astype(jnp.bfloat16)

    nb = 512
    spans = ow.shape[0] // nb

    def project(n):
        span = pl.ds(pl.multiple_of(n * nb, nb), nb)
        part[:, span] = lax.dot_general(
            ctx[...], ow[span, :], (((1,), (1,)), ((), ())),
            preferred_element_type=jnp.float32).astype(jnp.bfloat16)

    def flip(e):
        span = pl.ds(pl.multiple_of(e * tokens, tokens), tokens)
        u_t[:, span] = u_all[span, :].T

    def partial(c, e):
        span = pl.ds(pl.multiple_of(e * tokens, tokens), tokens)
        return jnp.dot(u_all[span, :], w_all[c], preferred_element_type=jnp.float32)

    def h_tick(n, e_of, held, copy, sends, first):
        @pl.when((n >= 0) & (n < CHUNKS * HOPS))
        def _():
            c, e = n // HOPS, e_of(lax.rem(n, HOPS))

            @pl.when(sends(e) & first)
            def _():
                held[c, e] = partial(c, e).astype(jnp.bfloat16)
                copy(c, e).start()

            @pl.when(sends(e) & jnp.logical_not(first))
            def _():
                mine = partial(c, e)
                copy(c, e).wait_recv()
                held[c, e] = (mine + held[c, e].astype(jnp.float32)).astype(jnp.bfloat16)
                copy(c, e).start()

    def weight_chunk(c):
        for j in range(1, INN):
            to = lax.rem(i + j, INN)
            span = pl.ds(pl.multiple_of(to * rows_w, rows_w), rows_w)
            g_send[c, j - 1] = jnp.dot(
                u_t[span, :], a_all[c], preferred_element_type=jnp.float32).astype(jnp.bfloat16)
            gx(c, j).start()
        span = pl.ds(pl.multiple_of(i * rows_w, rows_w), rows_w)
        wg_out[:, cols(c)] = jnp.dot(
            u_t[span, :], a_all[c], preferred_element_type=jnp.float32)

    head_ticks = -(-heads // HEADS_TICK)
    span_ticks = -(-spans // SPANS_TICK)

    def tick(k):
        c0 = k // HOPS

        @pl.when((lax.rem(k, HOPS) == 0) & (c0 < CHUNKS))
        def _():
            own_w(c0).wait()
            for j in range(1, INN):
                wx(c0, j).wait_recv()

        h_tick(k - LAG * o, lambda s: OUT - 1 - s, h_right, h_r, lambda e: o < e, o == 0)
        h_tick(k - LAG * (OUT - 1 - o), lambda s: s, h_left, h_l, lambda e: o > e, o == OUT - 1)

        a_tick(k + AHEAD)

        @pl.when((lax.rem(k, HOPS) == 0) & (c0 < CHUNKS))
        def _():
            hid_out[:, cols(c0)] = partial(c0, o)

        @pl.when(k == 0)
        def _():
            loop(OUT, flip)

        ka = k + AHEAD - HOPS * LAG
        ca = ka // HOPS

        @pl.when((ka >= 0) & (lax.rem(ka, HOPS) == 0) & (ca < CHUNKS))
        def _():
            weight_chunk(ca)

        @pl.when(k < head_ticks)
        def _():
            for r in range(HEADS_TICK):
                head(jnp.minimum(k * HEADS_TICK + r, heads - 1))

        kp = k - head_ticks

        @pl.when((kp >= 0) & (kp < span_ticks))
        def _():
            for r in range(SPANS_TICK):
                project(jnp.minimum(kp * SPANS_TICK + r, spans - 1))

        @pl.when(kp == span_ticks)
        def _():
            for j in range(1, TEN):
                att(j).start()

        cf = c0 - LAG

        @pl.when((lax.rem(k, HOPS) == 0) & (cf >= 0))
        def _():
            @pl.when(o > 0)
            def _():
                h_r(cf, o).wait_recv()
                hid_out[:, cols(cf)] += h_right[cf, o].astype(jnp.float32)

            @pl.when(o < OUT - 1)
            def _():
                h_l(cf, o).wait_recv()
                hid_out[:, cols(cf)] += h_left[cf, o].astype(jnp.float32)

            hid_out[:, cols(cf)] *= gelu_slope(pre[:, cols(cf)].astype(jnp.float32))

    loop((CHUNKS + LAG) * HOPS, tick)

    total = part[pl.ds(pl.multiple_of(t * rows, rows), rows), :].astype(jnp.float32)
    total = total + bias[...].astype(jnp.float32)[None, :]
    for j in range(1, TEN):
        att(j).wait_recv()
        total = total + att_recv[j - 1].astype(jnp.float32)
    att_out[...] = total

    factor = 1.0 / (OUT * INN)

    def finish(c):
        acc = wg_out[:, cols(c)]
        for j in range(1, INN):
            gx(c, j).wait_recv()
            acc = acc + g_recv[c, j - 1].astype(jnp.float32)
        wg_out[:, cols(c)] = acc * factor

    loop(CHUNKS, finish)

    for j in range(1, OUT):
        uz(j).wait_send()
    for j in range(OUT):
        for k in range(1, XS):
            ux(j, k).wait_send()
        for k in range(XS):
            uc(j, k).wait_send()
    for j in range(1, TEN):
        att(j).wait_send()

    def drain(c):
        for j in range(1, INN):
            wx(c, j).wait_send()
            gx(c, j).wait_send()
        for s in range(OUT - 1):
            er, el = OUT - 1 - s, s

            @pl.when(o < er)
            def _():
                h_r(c, er).wait_send()

            @pl.when(o > el)
            def _():
                h_l(c, el).wait_send()

            @pl.when((o < OUT - 1) & (o >= s))
            def _():
                a_right(c, s, s == 0).wait_send()

            @pl.when((o > 0) & (o + s <= OUT - 1))
            def _():
                a_left(c, s, s == 0).wait_send()

    loop(CHUNKS, drain)


def write_out(att, hid, wg, att_hbm, hid_hbm, wg_hbm, sem):
    copies = []
    for n, (src, dst) in enumerate(((att, att_hbm), (hid, hid_hbm), (wg, wg_hbm))):
        step = src.shape[0] // PIECES
        for p in range(PIECES):
            span = pl.ds(p * step, step)
            copies.append(pltpu.make_async_copy(src.at[span, :], dst.at[span, :], sem.at[n, p]))
    for copy in copies:
        copy.start()
    for copy in copies:
        copy.wait()


def body(sizes, qkv, segment_ids, out_weight, out_bias, upstream, pre_act, down_weight):
    OUT, INN, TEN = sizes
    rows, width = upstream.shape
    tokens, ff = pre_act.shape
    rows_w = down_weight.shape[0]
    fc = ff // CHUNKS
    bf, f32 = jnp.bfloat16, jnp.float32
    vmem = pl.BlockSpec(memory_space=pltpu.VMEM)
    anym = pl.BlockSpec(memory_space=pl.ANY)
    dma = lambda *shape: pltpu.SemaphoreType.DMA(shape)
    block = min(tokens, 4 * ROWS_DEV)
    held = 4 * (rows * width + tokens * ff + rows_w * ff)
    attention_out, act_grad, weight_grad = pl.pallas_call(
        functools.partial(kernel, sizes),
        out_shape=(
            pltpu.VMEM((rows, width), f32),
            pltpu.VMEM((tokens, ff), f32),
            pltpu.VMEM((rows_w, ff), f32),
        ),
        in_specs=[anym, vmem, anym, vmem, anym, vmem, anym],
        out_specs=(vmem, vmem, vmem),
        scratch_shapes=[
            pltpu.VMEM(qkv.shape, bf),
            pltpu.VMEM(out_weight.shape, bf),
            pltpu.VMEM((tokens, qkv.shape[2]), bf),
            pltpu.VMEM((tokens, width), bf),
            pltpu.VMEM((TEN - 1, rows, width), bf),
            pltpu.VMEM((OUT * tokens, INN * rows_w), bf),
            pltpu.VMEM((INN * rows_w, OUT * tokens), bf),
            pltpu.VMEM((CHUNKS, INN * rows_w, fc), bf),
            pltpu.VMEM((CHUNKS, OUT * tokens, fc), bf),
            pltpu.VMEM((CHUNKS, tokens, fc), bf),
            pltpu.VMEM((tokens // block, block, block), f32),
            pltpu.VMEM((CHUNKS, OUT, tokens, fc), bf),
            pltpu.VMEM((CHUNKS, OUT, tokens, fc), bf),
            pltpu.VMEM((CHUNKS, INN - 1, rows_w, fc), bf),
            pltpu.VMEM((CHUNKS, INN - 1, rows_w, fc), bf),
            dma(3), dma(1, CHUNKS), dma(TEN - 1), dma(TEN - 1),
            dma(OUT - 1), dma(OUT - 1),
            dma(OUT, max(TEN // 2 - 1, 1)), dma(OUT, max(TEN // 2 - 1, 1)),
            dma(OUT, TEN // 2), dma(OUT, TEN // 2),
            dma(CHUNKS, INN - 1), dma(CHUNKS, INN - 1),
            dma(CHUNKS, OUT - 1), dma(CHUNKS, OUT - 1),
            dma(CHUNKS, OUT - 1), dma(CHUNKS, OUT - 1),
            dma(CHUNKS, OUT), dma(CHUNKS, OUT),
            dma(CHUNKS, OUT), dma(CHUNKS, OUT),
            dma(CHUNKS, INN - 1), dma(CHUNKS, INN - 1),
        ],
        compiler_params=pltpu.CompilerParams(
            has_side_effects=True, vmem_limit_bytes=64_000_000 - held),
        name="layer",
    )(qkv, segment_ids, out_weight, out_bias, upstream, pre_act, down_weight)
    results = tuple(
        pltpu.with_memory_space_constraint(r, pltpu.VMEM)
        for r in (attention_out, act_grad, weight_grad))
    return pl.pallas_call(
        write_out,
        out_shape=tuple(jax.ShapeDtypeStruct(r.shape, f32) for r in results),
        in_specs=[vmem] * 3,
        out_specs=(anym,) * 3,
        scratch_shapes=[dma(3, PIECES)],
        compiler_params=pltpu.CompilerParams(vmem_limit_bytes=2**20),
        name="write_out",
    )(*results)


def solution(mesh):
    dp, tensor = mesh.shape["dp"], mesh.shape["tensor"]
    inner = 2 ** ((dp.bit_length() - 1) // 2)
    return jax.shard_map(
        functools.partial(body, (dp // inner, inner, tensor)),
        mesh=mesh,
        in_specs=(
            P(None, "dp", "tensor"),
            P("dp", None, None),
            P(None, "tensor"),
            P(),
            P(("dp", "tensor"), None),
            P("dp", "tensor"),
            P("dp", "tensor"),
        ),
        out_specs=(P(("dp", "tensor"), None), P("dp", "tensor"), P("dp", "tensor")),
        check_vma=False,
    )
```

```python
import functools
import math

import jax
import jax.numpy as jnp
from jax import lax
from jax.experimental import pallas as pl
from jax.experimental.pallas import tpu as pltpu
from jax.sharding import PartitionSpec as P

HEAD = 128
ROWS_DEV = 64
CHUNKS = 8
GROUP = 4
DELAY = 2
PIECES = 4

root_half = 1.0 / math.sqrt(2.0)
inv_root_tau = 1.0 / math.sqrt(2.0 * math.pi)


def gelu_exact(argument):
    return 0.5 * argument * (1.0 + lax.erf(argument * root_half))


def gelu_slope(argument):
    return (
        0.5 * (1.0 + lax.erf(argument * root_half))
        + argument * jnp.exp(-0.5 * argument * argument) * inv_root_tau
    )


def kernel(
    sizes,
    qkv_hbm, segments, ow_hbm, bias, up_hbm, pre_hbm, w_hbm,
    att_out, hid_out, wg_out,
    qkv, ow, ctx, part, att_recv,
    u_all, u_t, w_all, a_all, pre, same_ref, h_right, h_left, g_send, g_recv,
    local_sem, loc_wa, att_s, att_r,
    uz_s, uz_r, ux_s, ux_r, uc_s, uc_r,
    w_s, w_r, ar_s, ar_r, al_s, al_r,
    hr_s, hr_r, hl_s, hl_r, g_s, g_r,
):
    OUT, INN, TEN = sizes
    XS = TEN // 2
    g = lax.axis_index("dp")
    t = lax.axis_index("tensor")
    o, i = g // INN, lax.rem(g, INN)
    x, core = t // 2, lax.rem(t, 2)
    rows_w, ff = w_hbm.shape
    rows = up_hbm.shape[0]
    tokens = rows * TEN
    fc = ff // CHUNKS
    dcols = rows_w * INN
    HOPS = OUT - 1

    def remote(src, dst, ssem, rsem, dp, tensor):
        return pltpu.make_async_remote_copy(
            src_ref=src, dst_ref=dst, send_sem=ssem, recv_sem=rsem,
            device_id={"dp": dp, "tensor": tensor},
            device_id_type=pl.DeviceIdType.MESH,
        )

    def cols(c):
        return pl.ds(pl.multiple_of(c * fc, fc), fc)

    def u_rows(oo, tt):
        return u_all.at[pl.ds(pl.multiple_of((oo * TEN + tt) * rows, rows), rows), :]

    def a_rows(c, oo):
        return a_all.at[c, pl.ds(pl.multiple_of(oo * tokens, tokens), tokens), :]

    def w_rows(c, ii):
        return w_all.at[c, pl.ds(pl.multiple_of(ii * rows_w, rows_w), rows_w), :]

    def uz(j):
        to = lax.rem(o + j, OUT)
        return remote(
            up_hbm.at[:, pl.ds(pl.multiple_of(to * dcols, dcols), dcols)],
            u_rows(o, t), uz_s.at[j - 1], uz_r.at[j - 1], to * INN + i, t,
        )

    def ux(j, k):
        block = u_rows(lax.rem(o - j + OUT, OUT), t)
        return remote(block, block, ux_s.at[j, k - 1], ux_r.at[j, k - 1], g,
                      lax.rem(x + k, XS) * 2 + core)

    def uc(j, k):
        block = u_rows(lax.rem(o - j + OUT, OUT), lax.rem(x - k + XS, XS) * 2 + core)
        return remote(block, block, uc_s.at[j, k], uc_r.at[j, k], g, x * 2 + 1 - core)

    def wx(c, j):
        return remote(w_hbm.at[:, cols(c)], w_rows(c, i), w_s.at[c, j - 1], w_r.at[c, j - 1],
                      o * INN + lax.rem(i + j, INN), t)

    def a_right(c, s):
        block = a_rows(c, jnp.maximum(o - s, 0))
        return remote(block, block, ar_s.at[c, s], ar_r.at[c, s],
                      jnp.minimum(o + 1, OUT - 1) * INN + i, t)

    def a_left(c, s):
        block = a_rows(c, jnp.minimum(o + s, OUT - 1))
        return remote(block, block, al_s.at[c, s], al_r.at[c, s],
                      jnp.maximum(o - 1, 0) * INN + i, t)

    def h_r(c, e):
        return remote(h_right.at[c, e], h_right.at[c, e], hr_s.at[c, e], hr_r.at[c, e],
                      jnp.minimum(o + 1, OUT - 1) * INN + i, t)

    def h_l(c, e):
        return remote(h_left.at[c, e], h_left.at[c, e], hl_s.at[c, e], hl_r.at[c, e],
                      jnp.maximum(o - 1, 0) * INN + i, t)

    def gx(c, j):
        return remote(g_send.at[c, j - 1], g_recv.at[c, j - 1], g_s.at[c, j - 1], g_r.at[c, j - 1],
                      o * INN + lax.rem(i + j, INN), t)

    def att(j):
        to = lax.rem(t + j, TEN)
        return remote(part.at[pl.ds(pl.multiple_of(to * rows, rows), rows), :],
                      att_recv.at[j - 1], att_s.at[j - 1], att_r.at[j - 1], g, to)

    def own_w(c):
        return pltpu.make_async_copy(w_hbm.at[:, cols(c)], w_rows(c, i), loc_wa.at[0, c])

    def loop(count, fn):
        def step(index, carry):
            fn(index)
            return carry
        lax.fori_loop(0, count, step, 0)

    own_u = pltpu.make_async_copy(
        up_hbm.at[:, pl.ds(pl.multiple_of(o * dcols, dcols), dcols)], u_rows(o, t), local_sem.at[0])
    load_qkv = pltpu.make_async_copy(qkv_hbm, qkv, local_sem.at[1])
    load_ow = pltpu.make_async_copy(ow_hbm, ow, local_sem.at[2])

    load_pre = pltpu.make_async_copy(pre_hbm, pre, local_sem.at[3])

    for j in range(1, OUT):
        uz(j).start()
    load_pre.start()
    own_u.start()

    def start_w(c):
        for j in range(1, INN):
            wx(c, j).start()
        own_w(c).start()

    loop(CHUNKS, start_w)
    load_qkv.start()
    load_ow.start()

    right = (o, lambda p: p, a_right, ar_r, h_right, h_r)
    left = (OUT - 1 - o, lambda p: OUT - 1 - p, a_left, al_r, h_left, h_l)

    def a_wait(direction, c, s):
        r, place, _, arrived, _, _ = direction
        got = a_rows(c, place(jnp.maximum(r - s, 0)))
        remote(got, got, arrived.at[c, s - 1], arrived.at[c, s - 1], g, t).wait_recv()

    def a_item(direction, n):
        r, _, copy, _, _, _ = direction
        turn = (r + 1) * GROUP
        rest = lax.rem(n, turn)
        s = rest // GROUP
        c = n // turn * GROUP + lax.rem(rest, GROUP)

        @pl.when((r < OUT - 1) & (n < (r + 1) * CHUNKS))
        def _():
            @pl.when(s > 0)
            def _():
                a_wait(direction, c, s)
            copy(c, s).start()

    def activate(c):
        act = gelu_exact(pre[:, cols(c)].astype(jnp.float32)).astype(jnp.bfloat16)
        a_all[c, pl.ds(pl.multiple_of(o * tokens, tokens), tokens), :] = act

    def open_group(n):
        activate(n)
        a_item(right, n)
        a_item(left, n)

    load_pre.wait()
    loop(GROUP, open_group)
    own_u.wait()
    for k in range(1, XS):
        ux(0, k).start()
    uc(0, 0).start()
    loop(CHUNKS - GROUP, lambda n: activate(n + GROUP))

    heads = qkv.shape[2] // HEAD
    block = min(tokens, 4 * ROWS_DEV)
    scale = 1.0 / math.sqrt(HEAD)

    labels = segments[0].astype(jnp.float32)
    packs, length = labels.shape
    spread = (
        lax.rem(lax.broadcasted_iota(jnp.int32, (length, tokens), 1), length)
        == lax.broadcasted_iota(jnp.int32, (length, tokens), 0)
    ).astype(jnp.float32)
    wide = jnp.dot(labels, spread, preferred_element_type=jnp.float32)
    pack = lax.broadcasted_iota(jnp.int32, (packs, tokens), 0)
    here = lax.broadcasted_iota(jnp.int32, (packs, tokens), 1) // length == pack
    name = jnp.sum(
        jnp.where(here, wide + 2.0 * pack.astype(jnp.float32), 0.0), axis=0, keepdims=True)
    for b in range(tokens // block):
        across = jnp.broadcast_to(name[:, b * block : (b + 1) * block], (block, block))
        same_ref[b] = (across == across.T).astype(jnp.float32)

    def head(h):
        lanes = pl.ds(pl.multiple_of(h * HEAD, HEAD), HEAD)
        for b in range(tokens // block):
            mine = slice(b * block, (b + 1) * block)
            same = same_ref[b] > 0.5
            scores = lax.dot_general(
                qkv[0, mine, lanes], qkv[1, mine, lanes], (((1,), (1,)), ((), ())),
                preferred_element_type=jnp.float32) * scale
            masked = jnp.where(same, scores, -1e30)
            top = jnp.max(masked, axis=1, keepdims=True)
            exponent = jnp.where(same, jnp.exp(masked - top), 0.0)
            weights = (exponent / jnp.sum(exponent, axis=1, keepdims=True)).astype(jnp.bfloat16)
            ctx[mine, lanes] = jnp.dot(
                weights, qkv[2, mine, lanes], preferred_element_type=jnp.float32
            ).astype(jnp.bfloat16)

    nb = 512
    spans = ow.shape[0] // nb

    def project(n):
        span = pl.ds(pl.multiple_of(n * nb, nb), nb)
        part[:, span] = lax.dot_general(
            ctx[...], ow[span, :], (((1,), (1,)), ((), ())),
            preferred_element_type=jnp.float32).astype(jnp.bfloat16)

    def flip(e):
        span = pl.ds(pl.multiple_of(e * tokens, tokens), tokens)
        u_t[:, span] = u_all[span, :].T

    def partial(c, e):
        span = pl.ds(pl.multiple_of(e * tokens, tokens), tokens)
        return jnp.dot(u_all[span, :], w_all[c], preferred_element_type=jnp.float32)

    def h_item(direction, n):
        r, place, _, _, held, copy = direction
        m = n - (r + 1) * CHUNKS
        e = place(OUT - 1 - m // CHUNKS)
        c = lax.rem(m, CHUNKS)

        @pl.when((m >= 0) & (r == 0))
        def _():
            held[c, e] = partial(c, e).astype(jnp.bfloat16)
            copy(c, e).start()

        @pl.when((m >= 0) & (r > 0) & (r < OUT - 1))
        def _():
            mine = partial(c, e)
            copy(c, e).wait_recv()
            held[c, e] = (mine + held[c, e].astype(jnp.float32)).astype(jnp.bfloat16)
            copy(c, e).start()

    def weight_chunk(c):
        for direction in (right, left):
            @pl.when(direction[0] == OUT - 1)
            def _():
                for s in range(1, OUT):
                    a_wait(direction, c, s)
        for j in range(1, INN):
            to = lax.rem(i + j, INN)
            span = pl.ds(pl.multiple_of(to * rows_w, rows_w), rows_w)
            g_send[c, j - 1] = jnp.dot(
                u_t[span, :], a_all[c], preferred_element_type=jnp.float32).astype(jnp.bfloat16)
            gx(c, j).start()
        span = pl.ds(pl.multiple_of(i * rows_w, rows_w), rows_w)
        wg_out[:, cols(c)] = jnp.dot(
            u_t[span, :], a_all[c], preferred_element_type=jnp.float32)

    load_qkv.wait()
    loop(heads, head)

    for j in range(1, OUT):
        uz(j).wait_recv()
        for k in range(1, XS):
            ux(j, k).start()
        uc(j, 0).start()
    for j in range(OUT):
        for k in range(1, XS):
            ux(j, k).wait_recv()
            uc(j, k).start()
    for j in range(OUT):
        for k in range(XS):
            uc(j, k).wait_recv()
    loop(OUT, flip)
    load_ow.wait()

    def tick(k):
        n = k + GROUP
        first = n - CHUNKS

        @pl.when((first >= 0) & (first < CHUNKS))
        def _():
            own_w(first).wait()
            for j in range(1, INN):
                wx(first, j).wait_recv()

        for direction in (right, left):
            a_item(direction, n)
            h_item(direction, n)

        @pl.when((first >= 0) & (first < CHUNKS))
        def _():
            hid_out[:, cols(first)] = partial(first, o)

        @pl.when(k < spans)
        def _():
            project(k)

        @pl.when(k == spans)
        def _():
            for j in range(1, TEN):
                att(j).start()

        m = n - 1 - DELAY - (OUT - 2) * GROUP
        turn = (OUT - 1) * GROUP
        rest = lax.rem(m, turn)

        @pl.when((m >= 0) & (rest < GROUP) & (m // turn * GROUP < CHUNKS))
        def _():
            weight_chunk(m // turn * GROUP + rest)

    loop(OUT * CHUNKS - GROUP, tick)

    total = part[pl.ds(pl.multiple_of(t * rows, rows), rows), :].astype(jnp.float32)
    total = total + bias[...].astype(jnp.float32)[None, :]
    for j in range(1, TEN):
        att(j).wait_recv()
        total = total + att_recv[j - 1].astype(jnp.float32)
    att_out[...] = total

    factor = 1.0 / (OUT * INN)

    for j in range(1, OUT):
        uz(j).wait_send()
    for j in range(OUT):
        for k in range(1, XS):
            ux(j, k).wait_send()
        for k in range(XS):
            uc(j, k).wait_send()
    for j in range(1, TEN):
        att(j).wait_send()

    def finish(c):
        acc = wg_out[:, cols(c)]
        for j in range(1, INN):
            gx(c, j).wait_recv()
            acc = acc + g_recv[c, j - 1].astype(jnp.float32)
        wg_out[:, cols(c)] = acc * factor
        slope = gelu_slope(pre[:, cols(c)].astype(jnp.float32))

        @pl.when(o > 0)
        def _():
            h_r(c, o).wait_recv()
            hid_out[:, cols(c)] += h_right[c, o].astype(jnp.float32)

        @pl.when(o < OUT - 1)
        def _():
            h_l(c, o).wait_recv()
            hid_out[:, cols(c)] += h_left[c, o].astype(jnp.float32)

        hid_out[:, cols(c)] *= slope

        for j in range(1, INN):
            wx(c, j).wait_send()
            gx(c, j).wait_send()
        for s in range(OUT - 1):
            er, el = OUT - 1 - s, s

            @pl.when(o < er)
            def _():
                h_r(c, er).wait_send()

            @pl.when(o > el)
            def _():
                h_l(c, el).wait_send()

            @pl.when((o < OUT - 1) & (o >= s))
            def _():
                a_right(c, s).wait_send()

            @pl.when((o > 0) & (o + s <= OUT - 1))
            def _():
                a_left(c, s).wait_send()

    loop(CHUNKS, finish)


def write_out(att, hid, wg, att_hbm, hid_hbm, wg_hbm, sem):
    copies = []
    for n, (src, dst) in enumerate(((att, att_hbm), (hid, hid_hbm), (wg, wg_hbm))):
        step = src.shape[0] // PIECES
        for p in range(PIECES):
            span = pl.ds(p * step, step)
            copies.append(pltpu.make_async_copy(src.at[span, :], dst.at[span, :], sem.at[n, p]))
    for copy in copies:
        copy.start()
    for copy in copies:
        copy.wait()


def body(sizes, qkv, segment_ids, out_weight, out_bias, upstream, pre_act, down_weight):
    OUT, INN, TEN = sizes
    rows, width = upstream.shape
    tokens, ff = pre_act.shape
    rows_w = down_weight.shape[0]
    fc = ff // CHUNKS
    bf, f32 = jnp.bfloat16, jnp.float32
    vmem = pl.BlockSpec(memory_space=pltpu.VMEM)
    anym = pl.BlockSpec(memory_space=pl.ANY)
    dma = lambda *shape: pltpu.SemaphoreType.DMA(shape)
    block = min(tokens, 4 * ROWS_DEV)
    held = 4 * (rows * width + tokens * ff + rows_w * ff)
    attention_out, act_grad, weight_grad = pl.pallas_call(
        functools.partial(kernel, sizes),
        out_shape=(
            pltpu.VMEM((rows, width), f32),
            pltpu.VMEM((tokens, ff), f32),
            pltpu.VMEM((rows_w, ff), f32),
        ),
        in_specs=[anym, vmem, anym, vmem, anym, anym, anym],
        out_specs=(vmem, vmem, vmem),
        scratch_shapes=[
            pltpu.VMEM(qkv.shape, bf),
            pltpu.VMEM(out_weight.shape, bf),
            pltpu.VMEM((tokens, qkv.shape[2]), bf),
            pltpu.VMEM((tokens, width), bf),
            pltpu.VMEM((TEN - 1, rows, width), bf),
            pltpu.VMEM((OUT * tokens, INN * rows_w), bf),
            pltpu.VMEM((INN * rows_w, OUT * tokens), bf),
            pltpu.VMEM((CHUNKS, INN * rows_w, fc), bf),
            pltpu.VMEM((CHUNKS, OUT * tokens, fc), bf),
            pltpu.VMEM((tokens, ff), bf),
            pltpu.VMEM((tokens // block, block, block), f32),
            pltpu.VMEM((CHUNKS, OUT, tokens, fc), bf),
            pltpu.VMEM((CHUNKS, OUT, tokens, fc), bf),
            pltpu.VMEM((CHUNKS, INN - 1, rows_w, fc), bf),
            pltpu.VMEM((CHUNKS, INN - 1, rows_w, fc), bf),
            dma(4), dma(1, CHUNKS), dma(TEN - 1), dma(TEN - 1),
            dma(OUT - 1), dma(OUT - 1),
            dma(OUT, max(TEN // 2 - 1, 1)), dma(OUT, max(TEN // 2 - 1, 1)),
            dma(OUT, TEN // 2), dma(OUT, TEN // 2),
            dma(CHUNKS, INN - 1), dma(CHUNKS, INN - 1),
            dma(CHUNKS, OUT - 1), dma(CHUNKS, OUT - 1),
            dma(CHUNKS, OUT - 1), dma(CHUNKS, OUT - 1),
            dma(CHUNKS, OUT), dma(CHUNKS, OUT),
            dma(CHUNKS, OUT), dma(CHUNKS, OUT),
            dma(CHUNKS, INN - 1), dma(CHUNKS, INN - 1),
        ],
        compiler_params=pltpu.CompilerParams(
            has_side_effects=True, vmem_limit_bytes=64_000_000 - held),
        name="layer",
    )(qkv, segment_ids, out_weight, out_bias, upstream, pre_act, down_weight)
    results = tuple(
        pltpu.with_memory_space_constraint(r, pltpu.VMEM)
        for r in (attention_out, act_grad, weight_grad))
    return pl.pallas_call(
        write_out,
        out_shape=tuple(jax.ShapeDtypeStruct(r.shape, f32) for r in results),
        in_specs=[vmem] * 3,
        out_specs=(anym,) * 3,
        scratch_shapes=[dma(3, PIECES)],
        compiler_params=pltpu.CompilerParams(vmem_limit_bytes=2**20),
        name="write_out",
    )(*results)


def solution(mesh):
    dp, tensor = mesh.shape["dp"], mesh.shape["tensor"]
    inner = 2 ** ((dp.bit_length() - 1) // 2)
    return jax.shard_map(
        functools.partial(body, (dp // inner, inner, tensor)),
        mesh=mesh,
        in_specs=(
            P(None, "dp", "tensor"),
            P("dp", None, None),
            P(None, "tensor"),
            P(),
            P(("dp", "tensor"), None),
            P("dp", "tensor"),
            P("dp", "tensor"),
        ),
        out_specs=(P(("dp", "tensor"), None), P("dp", "tensor"), P("dp", "tensor")),
        check_vma=False,
    )
```

```python
import functools
import math

import jax
import jax.numpy as jnp
from jax import lax
from jax.experimental import pallas as pl
from jax.experimental.pallas import tpu as pltpu
from jax.sharding import PartitionSpec as P

HEAD = 128
ROWS_DEV = 64
CHUNKS = 8
GROUP = 4
DELAY = 2
PIECES = 4

root_half = 1.0 / math.sqrt(2.0)
inv_root_tau = 1.0 / math.sqrt(2.0 * math.pi)


def gelu_exact(argument):
    return 0.5 * argument * (1.0 + lax.erf(argument * root_half))


def gelu_slope(argument):
    return (
        0.5 * (1.0 + lax.erf(argument * root_half))
        + argument * jnp.exp(-0.5 * argument * argument) * inv_root_tau
    )


def kernel(
    sizes,
    qkv_hbm, segments, ow_hbm, bias, up_hbm, pre_hbm, w_hbm,
    att_out, hid_out, wg_out,
    qkv, ow, ctx, part, att_recv,
    up, u_all, u_t, w_all, a_all, pre, same_ref, h_right, h_left, g_send, g_recv,
    local_sem, loc_wa, att_s, att_r,
    uz_s, uz_r, ux_s, ux_r, uc_s, uc_r,
    w_s, w_r, ar_s, ar_r, al_s, al_r,
    hr_s, hr_r, hl_s, hl_r, g_s, g_r,
):
    OUT, INN, TEN = sizes
    XS = TEN // 2
    g = lax.axis_index("dp")
    t = lax.axis_index("tensor")
    o, i = g // INN, lax.rem(g, INN)
    x, core = t // 2, lax.rem(t, 2)
    rows_w, ff = w_hbm.shape
    rows = up_hbm.shape[0]
    tokens = rows * TEN
    fc = ff // CHUNKS
    dcols = rows_w * INN
    HOPS = OUT - 1

    def remote(src, dst, ssem, rsem, dp, tensor):
        return pltpu.make_async_remote_copy(
            src_ref=src, dst_ref=dst, send_sem=ssem, recv_sem=rsem,
            device_id={"dp": dp, "tensor": tensor},
            device_id_type=pl.DeviceIdType.MESH,
        )

    def cols(c):
        return pl.ds(pl.multiple_of(c * fc, fc), fc)

    def u_rows(oo, tt):
        return u_all.at[pl.ds(pl.multiple_of((oo * TEN + tt) * rows, rows), rows), :]

    def a_rows(c, oo):
        return a_all.at[c, pl.ds(pl.multiple_of(oo * tokens, tokens), tokens), :]

    def w_rows(c, ii):
        return w_all.at[c, pl.ds(pl.multiple_of(ii * rows_w, rows_w), rows_w), :]

    def uz(j):
        to = lax.rem(o + j, OUT)
        return remote(
            up.at[:, pl.ds(pl.multiple_of(to * dcols, dcols), dcols)],
            u_rows(o, t), uz_s.at[j - 1], uz_r.at[j - 1], to * INN + i, t,
        )

    def ux(j, k):
        block = u_rows(lax.rem(o - j + OUT, OUT), t)
        return remote(block, block, ux_s.at[j, k - 1], ux_r.at[j, k - 1], g,
                      lax.rem(x + k, XS) * 2 + core)

    def uc(j, k):
        block = u_rows(lax.rem(o - j + OUT, OUT), lax.rem(x - k + XS, XS) * 2 + core)
        return remote(block, block, uc_s.at[j, k], uc_r.at[j, k], g, x * 2 + 1 - core)

    def wx(c, j):
        return remote(w_hbm.at[:, cols(c)], w_rows(c, i), w_s.at[c, j - 1], w_r.at[c, j - 1],
                      o * INN + lax.rem(i + j, INN), t)

    def a_right(c, s):
        block = a_rows(c, jnp.maximum(o - s, 0))
        return remote(block, block, ar_s.at[c, s], ar_r.at[c, s],
                      jnp.minimum(o + 1, OUT - 1) * INN + i, t)

    def a_left(c, s):
        block = a_rows(c, jnp.minimum(o + s, OUT - 1))
        return remote(block, block, al_s.at[c, s], al_r.at[c, s],
                      jnp.maximum(o - 1, 0) * INN + i, t)

    def h_r(c, e):
        return remote(h_right.at[c, e], h_right.at[c, e], hr_s.at[c, e], hr_r.at[c, e],
                      jnp.minimum(o + 1, OUT - 1) * INN + i, t)

    def h_l(c, e):
        return remote(h_left.at[c, e], h_left.at[c, e], hl_s.at[c, e], hl_r.at[c, e],
                      jnp.maximum(o - 1, 0) * INN + i, t)

    def gx(c, j):
        return remote(g_send.at[c, j - 1], g_recv.at[c, j - 1], g_s.at[c, j - 1], g_r.at[c, j - 1],
                      o * INN + lax.rem(i + j, INN), t)

    def att(j):
        to = lax.rem(t + j, TEN)
        return remote(part.at[pl.ds(pl.multiple_of(to * rows, rows), rows), :],
                      att_recv.at[j - 1], att_s.at[j - 1], att_r.at[j - 1], g, to)

    def own_w(c):
        return pltpu.make_async_copy(w_hbm.at[:, cols(c)], w_rows(c, i), loc_wa.at[0, c])

    def loop(count, fn):
        def step(index, carry):
            fn(index)
            return carry
        lax.fori_loop(0, count, step, 0)

    load_up = pltpu.make_async_copy(up_hbm, up, local_sem.at[0])
    load_qkv = pltpu.make_async_copy(qkv_hbm, qkv, local_sem.at[1])
    load_ow = pltpu.make_async_copy(ow_hbm, ow, local_sem.at[2])
    load_pre = pltpu.make_async_copy(pre_hbm, pre, local_sem.at[3])

    partners = (
        [(lax.rem(o + j, OUT) * INN + i, t) for j in range(1, OUT)]
        + [(o * INN + lax.rem(i + j, INN), t) for j in range(1, INN)]
        + [(g, lax.rem(t + j, TEN)) for j in range(1, TEN)])
    barrier = pltpu.get_barrier_semaphore()
    for dp, tensor in partners:
        pl.semaphore_signal(barrier, inc=1, device_id={"dp": dp, "tensor": tensor},
                            device_id_type=pl.DeviceIdType.MESH)

    load_up.start()
    load_pre.start()
    load_up.wait()
    pl.semaphore_wait(barrier, len(partners))
    for j in range(1, OUT):
        uz(j).start()

    def start_w(c):
        for j in range(1, INN):
            wx(c, j).start()
        own_w(c).start()

    loop(CHUNKS, start_w)
    load_qkv.start()
    load_ow.start()
    u_all[pl.ds(pl.multiple_of((o * TEN + t) * rows, rows), rows), :] = (
        up[:, pl.ds(pl.multiple_of(o * dcols, dcols), dcols)])

    right = (o, lambda p: p, a_right, ar_r, h_right, h_r)
    left = (OUT - 1 - o, lambda p: OUT - 1 - p, a_left, al_r, h_left, h_l)

    def a_wait(direction, c, s):
        r, place, _, arrived, _, _ = direction
        got = a_rows(c, place(jnp.maximum(r - s, 0)))
        remote(got, got, arrived.at[c, s - 1], arrived.at[c, s - 1], g, t).wait_recv()

    def a_item(direction, n):
        r, _, copy, _, _, _ = direction
        turn = (r + 1) * GROUP
        rest = lax.rem(n, turn)
        s = rest // GROUP
        c = n // turn * GROUP + lax.rem(rest, GROUP)

        @pl.when((r < OUT - 1) & (n < (r + 1) * CHUNKS))
        def _():
            @pl.when(s > 0)
            def _():
                a_wait(direction, c, s)
            copy(c, s).start()

    def activate(c):
        act = gelu_exact(pre[:, cols(c)].astype(jnp.float32)).astype(jnp.bfloat16)
        a_all[c, pl.ds(pl.multiple_of(o * tokens, tokens), tokens), :] = act

    def open_group(n):
        activate(n)
        a_item(right, n)
        a_item(left, n)

    load_pre.wait()
    loop(GROUP, open_group)
    for k in range(1, XS):
        ux(0, k).start()
    uc(0, 0).start()
    loop(CHUNKS - GROUP, lambda n: activate(n + GROUP))

    heads = qkv.shape[2] // HEAD
    block = min(tokens, 4 * ROWS_DEV)
    scale = 1.0 / math.sqrt(HEAD)

    labels = segments[0].astype(jnp.float32)
    packs, length = labels.shape
    spread = (
        lax.rem(lax.broadcasted_iota(jnp.int32, (length, tokens), 1), length)
        == lax.broadcasted_iota(jnp.int32, (length, tokens), 0)
    ).astype(jnp.float32)
    wide = jnp.dot(labels, spread, preferred_element_type=jnp.float32)
    pack = lax.broadcasted_iota(jnp.int32, (packs, tokens), 0)
    here = lax.broadcasted_iota(jnp.int32, (packs, tokens), 1) // length == pack
    name = jnp.sum(
        jnp.where(here, wide + 2.0 * pack.astype(jnp.float32), 0.0), axis=0, keepdims=True)
    for b in range(tokens // block):
        across = jnp.broadcast_to(name[:, b * block : (b + 1) * block], (block, block))
        same_ref[b] = (across == across.T).astype(jnp.float32)

    def head(h):
        lanes = pl.ds(pl.multiple_of(h * HEAD, HEAD), HEAD)
        for b in range(tokens // block):
            mine = slice(b * block, (b + 1) * block)
            same = same_ref[b] > 0.5
            scores = lax.dot_general(
                qkv[0, mine, lanes], qkv[1, mine, lanes], (((1,), (1,)), ((), ())),
                preferred_element_type=jnp.float32) * scale
            masked = jnp.where(same, scores, -1e30)
            top = jnp.max(masked, axis=1, keepdims=True)
            exponent = jnp.where(same, jnp.exp(masked - top), 0.0)
            weights = (exponent / jnp.sum(exponent, axis=1, keepdims=True)).astype(jnp.bfloat16)
            ctx[mine, lanes] = jnp.dot(
                weights, qkv[2, mine, lanes], preferred_element_type=jnp.float32
            ).astype(jnp.bfloat16)

    nb = 512
    spans = ow.shape[0] // nb

    def project(n):
        span = pl.ds(pl.multiple_of(n * nb, nb), nb)
        part[:, span] = lax.dot_general(
            ctx[...], ow[span, :], (((1,), (1,)), ((), ())),
            preferred_element_type=jnp.float32).astype(jnp.bfloat16)

    def flip(e):
        span = pl.ds(pl.multiple_of(e * tokens, tokens), tokens)
        u_t[:, span] = u_all[span, :].T

    def partial(c, e):
        span = pl.ds(pl.multiple_of(e * tokens, tokens), tokens)
        return jnp.dot(u_all[span, :], w_all[c], preferred_element_type=jnp.float32)

    def h_item(direction, n):
        r, place, _, _, held, copy = direction
        m = n - (r + 1) * CHUNKS
        e = place(OUT - 1 - m // CHUNKS)
        c = lax.rem(m, CHUNKS)

        @pl.when((m >= 0) & (r == 0))
        def _():
            held[c, e] = partial(c, e).astype(jnp.bfloat16)
            copy(c, e).start()

        @pl.when((m >= 0) & (r > 0) & (r < OUT - 1))
        def _():
            mine = partial(c, e)
            copy(c, e).wait_recv()
            held[c, e] = (mine + held[c, e].astype(jnp.float32)).astype(jnp.bfloat16)
            copy(c, e).start()

    def weight_chunk(c):
        for direction in (right, left):
            @pl.when(direction[0] == OUT - 1)
            def _():
                for s in range(1, OUT):
                    a_wait(direction, c, s)
        for j in range(1, INN):
            to = lax.rem(i + j, INN)
            span = pl.ds(pl.multiple_of(to * rows_w, rows_w), rows_w)
            g_send[c, j - 1] = jnp.dot(
                u_t[span, :], a_all[c], preferred_element_type=jnp.float32).astype(jnp.bfloat16)
            gx(c, j).start()
        span = pl.ds(pl.multiple_of(i * rows_w, rows_w), rows_w)
        wg_out[:, cols(c)] = jnp.dot(
            u_t[span, :], a_all[c], preferred_element_type=jnp.float32)

    load_qkv.wait()
    loop(heads, head)

    for j in range(1, OUT):
        uz(j).wait_recv()
        for k in range(1, XS):
            ux(j, k).start()
        uc(j, 0).start()
    for j in range(OUT):
        for k in range(1, XS):
            ux(j, k).wait_recv()
            uc(j, k).start()
    for j in range(OUT):
        for k in range(XS):
            uc(j, k).wait_recv()
    loop(OUT, flip)
    load_ow.wait()

    def tick(k):
        n = k + GROUP
        first = n - CHUNKS

        @pl.when((first >= 0) & (first < CHUNKS))
        def _():
            own_w(first).wait()
            for j in range(1, INN):
                wx(first, j).wait_recv()

        for direction in (right, left):
            a_item(direction, n)
            h_item(direction, n)

        @pl.when((first >= 0) & (first < CHUNKS))
        def _():
            hid_out[:, cols(first)] = partial(first, o)

        @pl.when(k < spans)
        def _():
            project(k)

        @pl.when(k == spans)
        def _():
            for j in range(1, TEN):
                att(j).start()

        m = n - 1 - DELAY - (OUT - 2) * GROUP
        turn = (OUT - 1) * GROUP
        rest = lax.rem(m, turn)

        @pl.when((m >= 0) & (rest < GROUP) & (m // turn * GROUP < CHUNKS))
        def _():
            weight_chunk(m // turn * GROUP + rest)

    loop(OUT * CHUNKS - GROUP, tick)

    total = part[pl.ds(pl.multiple_of(t * rows, rows), rows), :].astype(jnp.float32)
    total = total + bias[...].astype(jnp.float32)[None, :]
    for j in range(1, TEN):
        att(j).wait_recv()
        total = total + att_recv[j - 1].astype(jnp.float32)
    att_out[...] = total

    factor = 1.0 / (OUT * INN)

    for j in range(1, OUT):
        uz(j).wait_send()
    for j in range(OUT):
        for k in range(1, XS):
            ux(j, k).wait_send()
        for k in range(XS):
            uc(j, k).wait_send()
    for j in range(1, TEN):
        att(j).wait_send()

    def finish(c):
        acc = wg_out[:, cols(c)]
        for j in range(1, INN):
            gx(c, j).wait_recv()
            acc = acc + g_recv[c, j - 1].astype(jnp.float32)
        wg_out[:, cols(c)] = acc * factor
        slope = gelu_slope(pre[:, cols(c)].astype(jnp.float32))

        @pl.when(o > 0)
        def _():
            h_r(c, o).wait_recv()
            hid_out[:, cols(c)] += h_right[c, o].astype(jnp.float32)

        @pl.when(o < OUT - 1)
        def _():
            h_l(c, o).wait_recv()
            hid_out[:, cols(c)] += h_left[c, o].astype(jnp.float32)

        hid_out[:, cols(c)] *= slope

        for j in range(1, INN):
            wx(c, j).wait_send()
            gx(c, j).wait_send()
        for s in range(OUT - 1):
            er, el = OUT - 1 - s, s

            @pl.when(o < er)
            def _():
                h_r(c, er).wait_send()

            @pl.when(o > el)
            def _():
                h_l(c, el).wait_send()

            @pl.when((o < OUT - 1) & (o >= s))
            def _():
                a_right(c, s).wait_send()

            @pl.when((o > 0) & (o + s <= OUT - 1))
            def _():
                a_left(c, s).wait_send()

    loop(CHUNKS, finish)


def write_out(att, hid, wg, att_hbm, hid_hbm, wg_hbm, sem):
    copies = []
    for n, (src, dst) in enumerate(((att, att_hbm), (hid, hid_hbm), (wg, wg_hbm))):
        step = src.shape[0] // PIECES
        for p in range(PIECES):
            span = pl.ds(p * step, step)
            copies.append(pltpu.make_async_copy(src.at[span, :], dst.at[span, :], sem.at[n, p]))
    for copy in copies:
        copy.start()
    for copy in copies:
        copy.wait()


def body(sizes, qkv, segment_ids, out_weight, out_bias, upstream, pre_act, down_weight):
    OUT, INN, TEN = sizes
    rows, width = upstream.shape
    tokens, ff = pre_act.shape
    rows_w = down_weight.shape[0]
    fc = ff // CHUNKS
    bf, f32 = jnp.bfloat16, jnp.float32
    vmem = pl.BlockSpec(memory_space=pltpu.VMEM)
    anym = pl.BlockSpec(memory_space=pl.ANY)
    dma = lambda *shape: pltpu.SemaphoreType.DMA(shape)
    block = min(tokens, 4 * ROWS_DEV)
    held = 4 * (rows * width + tokens * ff + rows_w * ff)
    attention_out, act_grad, weight_grad = pl.pallas_call(
        functools.partial(kernel, sizes),
        out_shape=(
            pltpu.VMEM((rows, width), f32),
            pltpu.VMEM((tokens, ff), f32),
            pltpu.VMEM((rows_w, ff), f32),
        ),
        in_specs=[anym, vmem, anym, vmem, anym, anym, anym],
        out_specs=(vmem, vmem, vmem),
        scratch_shapes=[
            pltpu.VMEM(qkv.shape, bf),
            pltpu.VMEM(out_weight.shape, bf),
            pltpu.VMEM((tokens, qkv.shape[2]), bf),
            pltpu.VMEM((tokens, width), bf),
            pltpu.VMEM((TEN - 1, rows, width), bf),
            pltpu.VMEM((rows, width), bf),
            pltpu.VMEM((OUT * tokens, INN * rows_w), bf),
            pltpu.VMEM((INN * rows_w, OUT * tokens), bf),
            pltpu.VMEM((CHUNKS, INN * rows_w, fc), bf),
            pltpu.VMEM((CHUNKS, OUT * tokens, fc), bf),
            pltpu.VMEM((tokens, ff), bf),
            pltpu.VMEM((tokens // block, block, block), f32),
            pltpu.VMEM((CHUNKS, OUT, tokens, fc), bf),
            pltpu.VMEM((CHUNKS, OUT, tokens, fc), bf),
            pltpu.VMEM((CHUNKS, INN - 1, rows_w, fc), bf),
            pltpu.VMEM((CHUNKS, INN - 1, rows_w, fc), bf),
            dma(4), dma(1, CHUNKS), dma(TEN - 1), dma(TEN - 1),
            dma(OUT - 1), dma(OUT - 1),
            dma(OUT, max(TEN // 2 - 1, 1)), dma(OUT, max(TEN // 2 - 1, 1)),
            dma(OUT, TEN // 2), dma(OUT, TEN // 2),
            dma(CHUNKS, INN - 1), dma(CHUNKS, INN - 1),
            dma(CHUNKS, OUT - 1), dma(CHUNKS, OUT - 1),
            dma(CHUNKS, OUT - 1), dma(CHUNKS, OUT - 1),
            dma(CHUNKS, OUT), dma(CHUNKS, OUT),
            dma(CHUNKS, OUT), dma(CHUNKS, OUT),
            dma(CHUNKS, INN - 1), dma(CHUNKS, INN - 1),
        ],
        compiler_params=pltpu.CompilerParams(
            has_side_effects=True, collective_id=0, vmem_limit_bytes=64_000_000 - held),
        name="layer",
    )(qkv, segment_ids, out_weight, out_bias, upstream, pre_act, down_weight)
    results = tuple(
        pltpu.with_memory_space_constraint(r, pltpu.VMEM)
        for r in (attention_out, act_grad, weight_grad))
    return pl.pallas_call(
        write_out,
        out_shape=tuple(jax.ShapeDtypeStruct(r.shape, f32) for r in results),
        in_specs=[vmem] * 3,
        out_specs=(anym,) * 3,
        scratch_shapes=[dma(3, PIECES)],
        compiler_params=pltpu.CompilerParams(vmem_limit_bytes=2**20),
        name="write_out",
    )(*results)


def solution(mesh):
    dp, tensor = mesh.shape["dp"], mesh.shape["tensor"]
    inner = 2 ** ((dp.bit_length() - 1) // 2)
    return jax.shard_map(
        functools.partial(body, (dp // inner, inner, tensor)),
        mesh=mesh,
        in_specs=(
            P(None, "dp", "tensor"),
            P("dp", None, None),
            P(None, "tensor"),
            P(),
            P(("dp", "tensor"), None),
            P("dp", "tensor"),
            P("dp", "tensor"),
        ),
        out_specs=(P(("dp", "tensor"), None), P("dp", "tensor"), P("dp", "tensor")),
        check_vma=False,
    )
```

```python
import functools
import math

import jax
import jax.numpy as jnp
from jax import lax
from jax.experimental import pallas as pl
from jax.experimental.pallas import tpu as pltpu
from jax.sharding import PartitionSpec as P

HEAD = 128
ROWS_DEV = 64
CHUNKS = 8
GROUP = 4
DELAY = 2
PIECES = 4

root_half = 1.0 / math.sqrt(2.0)
inv_root_tau = 1.0 / math.sqrt(2.0 * math.pi)


def gelu_exact(argument):
    return 0.5 * argument * (1.0 + lax.erf(argument * root_half))


def gelu_slope(argument):
    return (
        0.5 * (1.0 + lax.erf(argument * root_half))
        + argument * jnp.exp(-0.5 * argument * argument) * inv_root_tau
    )


def kernel(
    sizes,
    qkv_hbm, names_hbm, ow_hbm, bias_hbm, up_hbm, pre_hbm, w_hbm,
    att_out, hid_out, wg_out,
    segments, bias, qkv, ow, ctx, part, att_recv,
    up, u_all, u_t, w_all, a_all, pre, same_ref, h_right, h_left, g_send, g_recv,
    local_sem, loc_wa, att_s, att_r,
    uz_s, uz_r, ux_s, ux_r, uc_s, uc_r,
    w_s, w_r, ar_s, ar_r, al_s, al_r,
    hr_s, hr_r, hl_s, hl_r, g_s, g_r, far_sem,
):
    OUT, INN, TEN = sizes
    XS = TEN // 2
    g = lax.axis_index("dp")
    t = lax.axis_index("tensor")
    o, i = g // INN, lax.rem(g, INN)
    x, core = t // 2, lax.rem(t, 2)
    rows_w, ff = w_hbm.shape
    rows = up_hbm.shape[0]
    tokens = rows * TEN
    fc = ff // CHUNKS
    dcols = rows_w * INN
    HOPS = OUT - 1

    def remote(src, dst, ssem, rsem, dp, tensor):
        return pltpu.make_async_remote_copy(
            src_ref=src, dst_ref=dst, send_sem=ssem, recv_sem=rsem,
            device_id={"dp": dp, "tensor": tensor},
            device_id_type=pl.DeviceIdType.MESH,
        )

    def cols(c):
        return pl.ds(pl.multiple_of(c * fc, fc), fc)

    def u_rows(oo, tt):
        return u_all.at[pl.ds(pl.multiple_of((oo * TEN + tt) * rows, rows), rows), :]

    def a_rows(c, oo):
        return a_all.at[c, pl.ds(pl.multiple_of(oo * tokens, tokens), tokens), :]

    def w_rows(c, ii):
        return w_all.at[c, pl.ds(pl.multiple_of(ii * rows_w, rows_w), rows_w), :]

    def uz(j):
        to = lax.rem(o + j, OUT)
        return remote(
            up.at[:, pl.ds(pl.multiple_of(to * dcols, dcols), dcols)],
            u_rows(o, t), uz_s.at[j - 1], uz_r.at[j - 1], to * INN + i, t,
        )

    def ux(j, k):
        block = u_rows(lax.rem(o - j + OUT, OUT), t)
        return remote(block, block, ux_s.at[j, k - 1], ux_r.at[j, k - 1], g,
                      lax.rem(x + k, XS) * 2 + core)

    def uc(j, k):
        block = u_rows(lax.rem(o - j + OUT, OUT), lax.rem(x - k + XS, XS) * 2 + core)
        return remote(block, block, uc_s.at[j, k], uc_r.at[j, k], g, x * 2 + 1 - core)

    def wx(c, j):
        return remote(w_hbm.at[:, cols(c)], w_rows(c, i), w_s.at[c, j - 1], w_r.at[c, j - 1],
                      o * INN + lax.rem(i + j, INN), t)

    def a_right(c, s):
        block = a_rows(c, jnp.maximum(o - s, 0))
        return remote(block, block, ar_s.at[c, s], ar_r.at[c, s],
                      jnp.minimum(o + 1, OUT - 1) * INN + i, t)

    def a_left(c, s):
        block = a_rows(c, jnp.minimum(o + s, OUT - 1))
        return remote(block, block, al_s.at[c, s], al_r.at[c, s],
                      jnp.maximum(o - 1, 0) * INN + i, t)

    def h_r(c, e):
        return remote(h_right.at[c, e], h_right.at[c, e], hr_s.at[c, e], hr_r.at[c, e],
                      jnp.minimum(o + 1, OUT - 1) * INN + i, t)

    def h_l(c, e):
        return remote(h_left.at[c, e], h_left.at[c, e], hl_s.at[c, e], hl_r.at[c, e],
                      jnp.maximum(o - 1, 0) * INN + i, t)

    def gx(c, j):
        return remote(g_send.at[c, j - 1], g_recv.at[c, j - 1], g_s.at[c, j - 1], g_r.at[c, j - 1],
                      o * INN + lax.rem(i + j, INN), t)

    def att(j):
        to = lax.rem(t + j, TEN)
        return remote(part.at[pl.ds(pl.multiple_of(to * rows, rows), rows), :],
                      att_recv.at[j - 1], att_s.at[j - 1], att_r.at[j - 1], g, to)

    def own_w(c):
        return pltpu.make_async_copy(w_hbm.at[:, cols(c)], w_rows(c, i), loc_wa.at[0, c])

    def loop(count, fn):
        def step(index, carry):
            fn(index)
            return carry
        lax.fori_loop(0, count, step, 0)

    load_up = pltpu.make_async_copy(up_hbm, up, local_sem.at[0])
    load_qkv = pltpu.make_async_copy(qkv_hbm, qkv, local_sem.at[1])
    load_ow = pltpu.make_async_copy(ow_hbm, ow, local_sem.at[2])
    load_pre = pltpu.make_async_copy(pre_hbm, pre, local_sem.at[3])

    load_names = pltpu.make_async_copy(names_hbm, segments, local_sem.at[4])
    load_bias = pltpu.make_async_copy(bias_hbm, bias, local_sem.at[5])

    def signal(semaphore, dp, tensor):
        pl.semaphore_signal(semaphore, inc=1, device_id={"dp": dp, "tensor": tensor},
                            device_id_type=pl.DeviceIdType.MESH)

    load_up.start()
    load_pre.start()
    partners = (
        [(o * INN + lax.rem(i + j, INN), t) for j in range(1, INN)]
        + [(g, lax.rem(t + j, TEN)) for j in range(1, TEN)])
    barrier = pltpu.get_barrier_semaphore()

    @pl.when(o < OUT - 1)
    def _():
        signal(barrier, jnp.minimum(o + 1, OUT - 1) * INN + i, t)

    @pl.when(o > 0)
    def _():
        signal(barrier, jnp.maximum(o - 1, 0) * INN + i, t)

    for dp, tensor in partners:
        signal(barrier, dp, tensor)
    load_up.wait()
    sides = jnp.minimum(o, 1) + jnp.minimum(OUT - 1 - o, 1)
    pl.semaphore_wait(barrier, len(partners) + sides)

    def uz_near(to):
        return (to - o == 1) | (o - to == 1)

    for j in range(1, OUT):
        @pl.when(uz_near(lax.rem(o + j, OUT)))
        def _():
            uz(j).start()

    def start_w(c):
        for j in range(1, INN):
            wx(c, j).start()
        own_w(c).start()

    if OUT > 2:
        @pl.when(o >= 2)
        def _():
            pl.semaphore_wait(far_sem.at[0], 1)

        @pl.when((o >= 1) & (o <= OUT - 2))
        def _():
            signal(far_sem.at[0], jnp.minimum(o + 1, OUT - 1) * INN + i, t)

        loop(CHUNKS, start_w)

        @pl.when(o <= OUT - 3)
        def _():
            pl.semaphore_wait(far_sem.at[1], 1)

        @pl.when((o >= 1) & (o <= OUT - 2))
        def _():
            signal(far_sem.at[1], jnp.maximum(o - 1, 0) * INN + i, t)
    else:
        loop(CHUNKS, start_w)
    for j in range(1, OUT):
        @pl.when(jnp.logical_not(uz_near(lax.rem(o + j, OUT))))
        def _():
            uz(j).start()
    load_names.start()
    load_bias.start()
    load_qkv.start()
    load_ow.start()
    u_all[pl.ds(pl.multiple_of((o * TEN + t) * rows, rows), rows), :] = (
        up[:, pl.ds(pl.multiple_of(o * dcols, dcols), dcols)])

    right = (o, lambda p: p, a_right, ar_r, h_right, h_r)
    left = (OUT - 1 - o, lambda p: OUT - 1 - p, a_left, al_r, h_left, h_l)

    def a_wait(direction, c, s):
        r, place, _, arrived, _, _ = direction
        got = a_rows(c, place(jnp.maximum(r - s, 0)))
        remote(got, got, arrived.at[c, s - 1], arrived.at[c, s - 1], g, t).wait_recv()

    def a_item(direction, n):
        r, _, copy, _, _, _ = direction
        turn = (r + 1) * GROUP
        rest = lax.rem(n, turn)
        s = rest // GROUP
        c = n // turn * GROUP + lax.rem(rest, GROUP)

        @pl.when((r < OUT - 1) & (n < (r + 1) * CHUNKS))
        def _():
            @pl.when(s > 0)
            def _():
                a_wait(direction, c, s)
            copy(c, s).start()

    def activate(c):
        act = gelu_exact(pre[:, cols(c)].astype(jnp.float32)).astype(jnp.bfloat16)
        a_all[c, pl.ds(pl.multiple_of(o * tokens, tokens), tokens), :] = act

    def open_group(n):
        activate(n)
        a_item(right, n)
        a_item(left, n)

    load_pre.wait()
    loop(GROUP, open_group)
    for k in range(1, XS):
        ux(0, k).start()
    uc(0, 0).start()
    loop(CHUNKS - GROUP, lambda n: activate(n + GROUP))

    heads = qkv.shape[2] // HEAD
    block = min(tokens, 4 * ROWS_DEV)
    scale = 1.0 / math.sqrt(HEAD)

    load_names.wait()
    load_bias.wait()
    labels = segments[0].astype(jnp.float32)
    packs, length = labels.shape
    spread = (
        lax.rem(lax.broadcasted_iota(jnp.int32, (length, tokens), 1), length)
        == lax.broadcasted_iota(jnp.int32, (length, tokens), 0)
    ).astype(jnp.float32)
    wide = jnp.dot(labels, spread, preferred_element_type=jnp.float32)
    pack = lax.broadcasted_iota(jnp.int32, (packs, tokens), 0)
    here = lax.broadcasted_iota(jnp.int32, (packs, tokens), 1) // length == pack
    name = jnp.sum(
        jnp.where(here, wide + 2.0 * pack.astype(jnp.float32), 0.0), axis=0, keepdims=True)
    for b in range(tokens // block):
        across = jnp.broadcast_to(name[:, b * block : (b + 1) * block], (block, block))
        same_ref[b] = (across == across.T).astype(jnp.float32)

    def head(h):
        lanes = pl.ds(pl.multiple_of(h * HEAD, HEAD), HEAD)
        for b in range(tokens // block):
            mine = slice(b * block, (b + 1) * block)
            same = same_ref[b] > 0.5
            scores = lax.dot_general(
                qkv[0, mine, lanes], qkv[1, mine, lanes], (((1,), (1,)), ((), ())),
                preferred_element_type=jnp.float32) * scale
            masked = jnp.where(same, scores, -1e30)
            top = jnp.max(masked, axis=1, keepdims=True)
            exponent = jnp.where(same, jnp.exp(masked - top), 0.0)
            weights = (exponent / jnp.sum(exponent, axis=1, keepdims=True)).astype(jnp.bfloat16)
            ctx[mine, lanes] = jnp.dot(
                weights, qkv[2, mine, lanes], preferred_element_type=jnp.float32
            ).astype(jnp.bfloat16)

    nb = 512
    spans = ow.shape[0] // nb

    def project(n):
        span = pl.ds(pl.multiple_of(n * nb, nb), nb)
        part[:, span] = lax.dot_general(
            ctx[...], ow[span, :], (((1,), (1,)), ((), ())),
            preferred_element_type=jnp.float32).astype(jnp.bfloat16)

    def flip(e):
        span = pl.ds(pl.multiple_of(e * tokens, tokens), tokens)
        u_t[:, span] = u_all[span, :].T

    def partial(c, e):
        span = pl.ds(pl.multiple_of(e * tokens, tokens), tokens)
        return jnp.dot(u_all[span, :], w_all[c], preferred_element_type=jnp.float32)

    def h_item(direction, n):
        r, place, _, _, held, copy = direction
        m = n - (r + 1) * CHUNKS
        e = place(OUT - 1 - m // CHUNKS)
        c = lax.rem(m, CHUNKS)

        @pl.when((m >= 0) & (r == 0))
        def _():
            held[c, e] = partial(c, e).astype(jnp.bfloat16)
            copy(c, e).start()

        @pl.when((m >= 0) & (r > 0) & (r < OUT - 1))
        def _():
            mine = partial(c, e)
            copy(c, e).wait_recv()
            held[c, e] = (mine + held[c, e].astype(jnp.float32)).astype(jnp.bfloat16)
            copy(c, e).start()

    def weight_chunk(c):
        for direction in (right, left):
            @pl.when(direction[0] == OUT - 1)
            def _():
                for s in range(1, OUT):
                    a_wait(direction, c, s)
        for j in range(1, INN):
            to = lax.rem(i + j, INN)
            span = pl.ds(pl.multiple_of(to * rows_w, rows_w), rows_w)
            g_send[c, j - 1] = jnp.dot(
                u_t[span, :], a_all[c], preferred_element_type=jnp.float32).astype(jnp.bfloat16)
            gx(c, j).start()
        span = pl.ds(pl.multiple_of(i * rows_w, rows_w), rows_w)
        wg_out[:, cols(c)] = jnp.dot(
            u_t[span, :], a_all[c], preferred_element_type=jnp.float32)

    load_qkv.wait()
    loop(heads, head)

    for j in range(1, OUT):
        uz(j).wait_recv()
        for k in range(1, XS):
            ux(j, k).start()
        uc(j, 0).start()
    for j in range(OUT):
        for k in range(1, XS):
            ux(j, k).wait_recv()
            uc(j, k).start()
    for j in range(OUT):
        for k in range(XS):
            uc(j, k).wait_recv()
    loop(OUT, flip)
    load_ow.wait()

    def tick(k):
        n = k + GROUP
        first = n - CHUNKS

        @pl.when((first >= 0) & (first < CHUNKS))
        def _():
            own_w(first).wait()
            for j in range(1, INN):
                wx(first, j).wait_recv()

        for direction in (right, left):
            a_item(direction, n)
            h_item(direction, n)

        @pl.when((first >= 0) & (first < CHUNKS))
        def _():
            hid_out[:, cols(first)] = partial(first, o)

        @pl.when(k < spans)
        def _():
            project(k)

        @pl.when(k == spans)
        def _():
            for j in range(1, TEN):
                att(j).start()

        m = n - 1 - DELAY - (OUT - 2) * GROUP
        turn = (OUT - 1) * GROUP
        rest = lax.rem(m, turn)

        @pl.when((m >= 0) & (rest < GROUP) & (m // turn * GROUP < CHUNKS))
        def _():
            weight_chunk(m // turn * GROUP + rest)

    loop(OUT * CHUNKS - GROUP, tick)

    total = part[pl.ds(pl.multiple_of(t * rows, rows), rows), :].astype(jnp.float32)
    total = total + bias[...].astype(jnp.float32)[None, :]
    for j in range(1, TEN):
        att(j).wait_recv()
        total = total + att_recv[j - 1].astype(jnp.float32)
    att_out[...] = total

    factor = 1.0 / (OUT * INN)

    for j in range(1, OUT):
        uz(j).wait_send()
    for j in range(OUT):
        for k in range(1, XS):
            ux(j, k).wait_send()
        for k in range(XS):
            uc(j, k).wait_send()
    for j in range(1, TEN):
        att(j).wait_send()

    def finish(c):
        acc = wg_out[:, cols(c)]
        for j in range(1, INN):
            gx(c, j).wait_recv()
            acc = acc + g_recv[c, j - 1].astype(jnp.float32)
        wg_out[:, cols(c)] = acc * factor
        for j in range(1, INN):
            wx(c, j).wait_send()
            gx(c, j).wait_send()
        for s in range(OUT - 1):
            @pl.when((o < OUT - 1) & (o >= s))
            def _():
                a_right(c, s).wait_send()

            @pl.when((o > 0) & (o + s <= OUT - 1))
            def _():
                a_left(c, s).wait_send()

    loop(CHUNKS, finish)

    def close(c):
        slope = gelu_slope(pre[:, cols(c)].astype(jnp.float32))

        @pl.when(o == 0)
        def _():
            h_l(c, o).wait_recv()
            hid_out[:, cols(c)] = (
                hid_out[:, cols(c)] + h_left[c, o].astype(jnp.float32)) * slope

        @pl.when(o == OUT - 1)
        def _():
            h_r(c, o).wait_recv()
            hid_out[:, cols(c)] = (
                hid_out[:, cols(c)] + h_right[c, o].astype(jnp.float32)) * slope

        @pl.when((o > 0) & (o < OUT - 1))
        def _():
            h_r(c, o).wait_recv()
            h_l(c, o).wait_recv()
            hid_out[:, cols(c)] = (
                hid_out[:, cols(c)] + h_right[c, o].astype(jnp.float32)
                + h_left[c, o].astype(jnp.float32)) * slope

        for s in range(OUT - 1):
            er, el = OUT - 1 - s, s

            @pl.when(o < er)
            def _():
                h_r(c, er).wait_send()

            @pl.when(o > el)
            def _():
                h_l(c, el).wait_send()

    loop(CHUNKS, close)


def write_out(att, hid, wg, att_hbm, hid_hbm, wg_hbm, sem):
    copies = []
    for n, (src, dst) in enumerate(((att, att_hbm), (hid, hid_hbm), (wg, wg_hbm))):
        step = src.shape[0] // PIECES
        for p in range(PIECES):
            span = pl.ds(p * step, step)
            copies.append(pltpu.make_async_copy(src.at[span, :], dst.at[span, :], sem.at[n, p]))
    for copy in copies:
        copy.start()
    for copy in copies:
        copy.wait()


def body(sizes, qkv, segment_ids, out_weight, out_bias, upstream, pre_act, down_weight):
    OUT, INN, TEN = sizes
    rows, width = upstream.shape
    tokens, ff = pre_act.shape
    rows_w = down_weight.shape[0]
    fc = ff // CHUNKS
    bf, f32 = jnp.bfloat16, jnp.float32
    vmem = pl.BlockSpec(memory_space=pltpu.VMEM)
    anym = pl.BlockSpec(memory_space=pl.ANY)
    dma = lambda *shape: pltpu.SemaphoreType.DMA(shape)
    block = min(tokens, 4 * ROWS_DEV)
    held = 4 * (rows * width + tokens * ff + rows_w * ff)
    attention_out, act_grad, weight_grad = pl.pallas_call(
        functools.partial(kernel, sizes),
        out_shape=(
            pltpu.VMEM((rows, width), f32),
            pltpu.VMEM((tokens, ff), f32),
            pltpu.VMEM((rows_w, ff), f32),
        ),
        in_specs=[anym] * 7,
        out_specs=(vmem, vmem, vmem),
        scratch_shapes=[
            pltpu.VMEM(segment_ids.shape, segment_ids.dtype),
            pltpu.VMEM(out_bias.shape, bf),
            pltpu.VMEM(qkv.shape, bf),
            pltpu.VMEM(out_weight.shape, bf),
            pltpu.VMEM((tokens, qkv.shape[2]), bf),
            pltpu.VMEM((tokens, width), bf),
            pltpu.VMEM((TEN - 1, rows, width), bf),
            pltpu.VMEM((rows, width), bf),
            pltpu.VMEM((OUT * tokens, INN * rows_w), bf),
            pltpu.VMEM((INN * rows_w, OUT * tokens), bf),
            pltpu.VMEM((CHUNKS, INN * rows_w, fc), bf),
            pltpu.VMEM((CHUNKS, OUT * tokens, fc), bf),
            pltpu.VMEM((tokens, ff), bf),
            pltpu.VMEM((tokens // block, block, block), f32),
            pltpu.VMEM((CHUNKS, OUT, tokens, fc), bf),
            pltpu.VMEM((CHUNKS, OUT, tokens, fc), bf),
            pltpu.VMEM((CHUNKS, INN - 1, rows_w, fc), bf),
            pltpu.VMEM((CHUNKS, INN - 1, rows_w, fc), bf),
            dma(6), dma(1, CHUNKS), dma(TEN - 1), dma(TEN - 1),
            dma(OUT - 1), dma(OUT - 1),
            dma(OUT, max(TEN // 2 - 1, 1)), dma(OUT, max(TEN // 2 - 1, 1)),
            dma(OUT, TEN // 2), dma(OUT, TEN // 2),
            dma(CHUNKS, INN - 1), dma(CHUNKS, INN - 1),
            dma(CHUNKS, OUT - 1), dma(CHUNKS, OUT - 1),
            dma(CHUNKS, OUT - 1), dma(CHUNKS, OUT - 1),
            dma(CHUNKS, OUT), dma(CHUNKS, OUT),
            dma(CHUNKS, OUT), dma(CHUNKS, OUT),
            dma(CHUNKS, INN - 1), dma(CHUNKS, INN - 1),
            pltpu.SemaphoreType.REGULAR((2,)),
        ],
        compiler_params=pltpu.CompilerParams(
            has_side_effects=True, collective_id=0, vmem_limit_bytes=64_000_000 - held),
        name="layer",
    )(qkv, segment_ids, out_weight, out_bias, upstream, pre_act, down_weight)
    results = tuple(
        pltpu.with_memory_space_constraint(r, pltpu.VMEM)
        for r in (attention_out, act_grad, weight_grad))
    return pl.pallas_call(
        write_out,
        out_shape=tuple(jax.ShapeDtypeStruct(r.shape, f32) for r in results),
        in_specs=[vmem] * 3,
        out_specs=(anym,) * 3,
        scratch_shapes=[dma(3, PIECES)],
        compiler_params=pltpu.CompilerParams(vmem_limit_bytes=2**20),
        name="write_out",
    )(*results)


def solution(mesh):
    dp, tensor = mesh.shape["dp"], mesh.shape["tensor"]
    inner = 2 ** ((dp.bit_length() - 1) // 2)
    return jax.shard_map(
        functools.partial(body, (dp // inner, inner, tensor)),
        mesh=mesh,
        in_specs=(
            P(None, "dp", "tensor"),
            P("dp", None, None),
            P(None, "tensor"),
            P(),
            P(("dp", "tensor"), None),
            P("dp", "tensor"),
            P("dp", "tensor"),
        ),
        out_specs=(P(("dp", "tensor"), None), P("dp", "tensor"), P("dp", "tensor")),
        check_vma=False,
    )
```

```python
import functools
import math

import jax
import jax.numpy as jnp
from jax import lax
from jax.experimental import pallas as pl
from jax.experimental.pallas import tpu as pltpu
from jax.sharding import PartitionSpec as P

HEAD = 128
ROWS_DEV = 64
CHUNKS = 4
GROUP = 2
DELAY = 1
PIECES = 4

root_half = 1.0 / math.sqrt(2.0)
inv_root_tau = 1.0 / math.sqrt(2.0 * math.pi)


def gelu_exact(argument):
    return 0.5 * argument * (1.0 + lax.erf(argument * root_half))


def gelu_slope(argument):
    return (
        0.5 * (1.0 + lax.erf(argument * root_half))
        + argument * jnp.exp(-0.5 * argument * argument) * inv_root_tau
    )


def kernel(
    sizes,
    qkv_hbm, names_hbm, ow_hbm, bias_hbm, up_hbm, pre_hbm, w_hbm,
    att_out, hid_out, wg_out,
    segments, bias, qkv, ow, ctx, part, att_recv,
    up, u_all, u_t, w_all, a_all, pre, same_ref, h_right, h_left, g_send, g_recv,
    local_sem, loc_wa, att_s, att_r,
    uz_s, uz_r, ux_s, ux_r, uc_s, uc_r,
    w_s, w_r, ar_s, ar_r, al_s, al_r,
    hr_s, hr_r, hl_s, hl_r, g_s, g_r, far_sem,
):
    OUT, INN, TEN = sizes
    XS = TEN // 2
    g = lax.axis_index("dp")
    t = lax.axis_index("tensor")
    o, i = g // INN, lax.rem(g, INN)
    x, core = t // 2, lax.rem(t, 2)
    rows_w, ff = w_hbm.shape
    rows = up_hbm.shape[0]
    tokens = rows * TEN
    fc = ff // CHUNKS
    dcols = rows_w * INN
    HOPS = OUT - 1

    def remote(src, dst, ssem, rsem, dp, tensor):
        return pltpu.make_async_remote_copy(
            src_ref=src, dst_ref=dst, send_sem=ssem, recv_sem=rsem,
            device_id={"dp": dp, "tensor": tensor},
            device_id_type=pl.DeviceIdType.MESH,
        )

    def cols(c):
        return pl.ds(pl.multiple_of(c * fc, fc), fc)

    def u_rows(oo, tt):
        return u_all.at[pl.ds(pl.multiple_of((oo * TEN + tt) * rows, rows), rows), :]

    def a_rows(c, oo):
        return a_all.at[c, pl.ds(pl.multiple_of(oo * tokens, tokens), tokens), :]

    def w_rows(c, ii):
        return w_all.at[c, pl.ds(pl.multiple_of(ii * rows_w, rows_w), rows_w), :]

    def uz(j):
        to = lax.rem(o + j, OUT)
        return remote(
            up.at[:, pl.ds(pl.multiple_of(to * dcols, dcols), dcols)],
            u_rows(o, t), uz_s.at[j - 1], uz_r.at[j - 1], to * INN + i, t,
        )

    def ux(j, k):
        block = u_rows(lax.rem(o - j + OUT, OUT), t)
        return remote(block, block, ux_s.at[j, k - 1], ux_r.at[j, k - 1], g,
                      lax.rem(x + k, XS) * 2 + core)

    def uc(j, k):
        block = u_rows(lax.rem(o - j + OUT, OUT), lax.rem(x - k + XS, XS) * 2 + core)
        return remote(block, block, uc_s.at[j, k], uc_r.at[j, k], g, x * 2 + 1 - core)

    def wx(c, j):
        return remote(w_hbm.at[:, cols(c)], w_rows(c, i), w_s.at[c, j - 1], w_r.at[c, j - 1],
                      o * INN + lax.rem(i + j, INN), t)

    def a_right(c, s):
        block = a_rows(c, jnp.maximum(o - s, 0))
        return remote(block, block, ar_s.at[c, s], ar_r.at[c, s],
                      jnp.minimum(o + 1, OUT - 1) * INN + i, t)

    def a_left(c, s):
        block = a_rows(c, jnp.minimum(o + s, OUT - 1))
        return remote(block, block, al_s.at[c, s], al_r.at[c, s],
                      jnp.maximum(o - 1, 0) * INN + i, t)

    def h_r(c, e):
        return remote(h_right.at[c, e], h_right.at[c, e], hr_s.at[c, e], hr_r.at[c, e],
                      jnp.minimum(o + 1, OUT - 1) * INN + i, t)

    def h_l(c, e):
        return remote(h_left.at[c, e], h_left.at[c, e], hl_s.at[c, e], hl_r.at[c, e],
                      jnp.maximum(o - 1, 0) * INN + i, t)

    def gx(c, j):
        return remote(g_send.at[c, j - 1], g_recv.at[c, j - 1], g_s.at[c, j - 1], g_r.at[c, j - 1],
                      o * INN + lax.rem(i + j, INN), t)

    def att(j):
        to = lax.rem(t + j, TEN)
        return remote(part.at[pl.ds(pl.multiple_of(to * rows, rows), rows), :],
                      att_recv.at[j - 1], att_s.at[j - 1], att_r.at[j - 1], g, to)

    def own_w(c):
        return pltpu.make_async_copy(w_hbm.at[:, cols(c)], w_rows(c, i), loc_wa.at[0, c])

    def loop(count, fn):
        def step(index, carry):
            fn(index)
            return carry
        lax.fori_loop(0, count, step, 0)

    load_up = pltpu.make_async_copy(up_hbm, up, local_sem.at[0])
    load_qkv = pltpu.make_async_copy(qkv_hbm, qkv, local_sem.at[1])
    load_ow = pltpu.make_async_copy(ow_hbm, ow, local_sem.at[2])
    load_pre = pltpu.make_async_copy(pre_hbm, pre, local_sem.at[3])

    load_names = pltpu.make_async_copy(names_hbm, segments, local_sem.at[4])
    load_bias = pltpu.make_async_copy(bias_hbm, bias, local_sem.at[5])

    def signal(semaphore, dp, tensor):
        pl.semaphore_signal(semaphore, inc=1, device_id={"dp": dp, "tensor": tensor},
                            device_id_type=pl.DeviceIdType.MESH)

    load_up.start()
    load_pre.start()
    partners = (
        [(o * INN + lax.rem(i + j, INN), t) for j in range(1, INN)]
        + [(g, lax.rem(t + j, TEN)) for j in range(1, TEN)])
    barrier = pltpu.get_barrier_semaphore()

    @pl.when(o < OUT - 1)
    def _():
        signal(barrier, jnp.minimum(o + 1, OUT - 1) * INN + i, t)

    @pl.when(o > 0)
    def _():
        signal(barrier, jnp.maximum(o - 1, 0) * INN + i, t)

    for dp, tensor in partners:
        signal(barrier, dp, tensor)
    load_up.wait()
    sides = jnp.minimum(o, 1) + jnp.minimum(OUT - 1 - o, 1)
    pl.semaphore_wait(barrier, len(partners) + sides)

    def uz_near(to):
        return (to - o == 1) | (o - to == 1)

    for j in range(1, OUT):
        @pl.when(uz_near(lax.rem(o + j, OUT)))
        def _():
            uz(j).start()

    def start_w(c):
        for j in range(1, INN):
            wx(c, j).start()
        own_w(c).start()

    if OUT > 2:
        @pl.when(o >= 2)
        def _():
            pl.semaphore_wait(far_sem.at[0], 1)

        @pl.when((o >= 1) & (o <= OUT - 2))
        def _():
            signal(far_sem.at[0], jnp.minimum(o + 1, OUT - 1) * INN + i, t)

        loop(CHUNKS, start_w)

        @pl.when(o <= OUT - 3)
        def _():
            pl.semaphore_wait(far_sem.at[1], 1)

        @pl.when((o >= 1) & (o <= OUT - 2))
        def _():
            signal(far_sem.at[1], jnp.maximum(o - 1, 0) * INN + i, t)
    else:
        loop(CHUNKS, start_w)
    for j in range(1, OUT):
        @pl.when(jnp.logical_not(uz_near(lax.rem(o + j, OUT))))
        def _():
            uz(j).start()
    load_names.start()
    load_bias.start()
    load_qkv.start()
    load_ow.start()
    u_all[pl.ds(pl.multiple_of((o * TEN + t) * rows, rows), rows), :] = (
        up[:, pl.ds(pl.multiple_of(o * dcols, dcols), dcols)])

    right = (o, lambda p: p, a_right, ar_r, h_right, h_r)
    left = (OUT - 1 - o, lambda p: OUT - 1 - p, a_left, al_r, h_left, h_l)

    def a_wait(direction, c, s):
        r, place, _, arrived, _, _ = direction
        got = a_rows(c, place(jnp.maximum(r - s, 0)))
        remote(got, got, arrived.at[c, s - 1], arrived.at[c, s - 1], g, t).wait_recv()

    def a_item(direction, n):
        r, _, copy, _, _, _ = direction
        turn = (r + 1) * GROUP
        rest = lax.rem(n, turn)
        s = rest // GROUP
        c = n // turn * GROUP + lax.rem(rest, GROUP)

        @pl.when((r < OUT - 1) & (n < (r + 1) * CHUNKS))
        def _():
            @pl.when(s > 0)
            def _():
                a_wait(direction, c, s)
            copy(c, s).start()

    def activate(c):
        act = gelu_exact(pre[:, cols(c)].astype(jnp.float32)).astype(jnp.bfloat16)
        a_all[c, pl.ds(pl.multiple_of(o * tokens, tokens), tokens), :] = act

    def open_group(n):
        activate(n)
        a_item(right, n)
        a_item(left, n)

    load_pre.wait()
    loop(GROUP, open_group)
    for k in range(1, XS):
        ux(0, k).start()
    uc(0, 0).start()
    loop(CHUNKS - GROUP, lambda n: activate(n + GROUP))

    heads = qkv.shape[2] // HEAD
    block = min(tokens, 4 * ROWS_DEV)
    scale = 1.0 / math.sqrt(HEAD)

    load_names.wait()
    load_bias.wait()
    labels = segments[0].astype(jnp.float32)
    packs, length = labels.shape
    spread = (
        lax.rem(lax.broadcasted_iota(jnp.int32, (length, tokens), 1), length)
        == lax.broadcasted_iota(jnp.int32, (length, tokens), 0)
    ).astype(jnp.float32)
    wide = jnp.dot(labels, spread, preferred_element_type=jnp.float32)
    pack = lax.broadcasted_iota(jnp.int32, (packs, tokens), 0)
    here = lax.broadcasted_iota(jnp.int32, (packs, tokens), 1) // length == pack
    name = jnp.sum(
        jnp.where(here, wide + 2.0 * pack.astype(jnp.float32), 0.0), axis=0, keepdims=True)
    for b in range(tokens // block):
        across = jnp.broadcast_to(name[:, b * block : (b + 1) * block], (block, block))
        same_ref[b] = (across == across.T).astype(jnp.float32)

    def head(h):
        lanes = pl.ds(pl.multiple_of(h * HEAD, HEAD), HEAD)
        for b in range(tokens // block):
            mine = slice(b * block, (b + 1) * block)
            same = same_ref[b] > 0.5
            scores = lax.dot_general(
                qkv[0, mine, lanes], qkv[1, mine, lanes], (((1,), (1,)), ((), ())),
                preferred_element_type=jnp.float32) * scale
            masked = jnp.where(same, scores, -1e30)
            top = jnp.max(masked, axis=1, keepdims=True)
            exponent = jnp.where(same, jnp.exp(masked - top), 0.0)
            weights = (exponent / jnp.sum(exponent, axis=1, keepdims=True)).astype(jnp.bfloat16)
            ctx[mine, lanes] = jnp.dot(
                weights, qkv[2, mine, lanes], preferred_element_type=jnp.float32
            ).astype(jnp.bfloat16)

    nb = 512
    spans = ow.shape[0] // nb

    def project(n):
        span = pl.ds(pl.multiple_of(n * nb, nb), nb)
        part[:, span] = lax.dot_general(
            ctx[...], ow[span, :], (((1,), (1,)), ((), ())),
            preferred_element_type=jnp.float32).astype(jnp.bfloat16)

    def flip(e):
        span = pl.ds(pl.multiple_of(e * tokens, tokens), tokens)
        u_t[:, span] = u_all[span, :].T

    def partial(c, e):
        span = pl.ds(pl.multiple_of(e * tokens, tokens), tokens)
        return jnp.dot(u_all[span, :], w_all[c], preferred_element_type=jnp.float32)

    def h_item(direction, n):
        r, place, _, _, held, copy = direction
        m = n - (r + 1) * CHUNKS
        e = place(OUT - 1 - m // CHUNKS)
        c = lax.rem(m, CHUNKS)

        @pl.when((m >= 0) & (r == 0))
        def _():
            held[c, e] = partial(c, e).astype(jnp.bfloat16)
            copy(c, e).start()

        @pl.when((m >= 0) & (r > 0) & (r < OUT - 1))
        def _():
            mine = partial(c, e)
            copy(c, e).wait_recv()
            held[c, e] = (mine + held[c, e].astype(jnp.float32)).astype(jnp.bfloat16)
            copy(c, e).start()

    def weight_chunk(c):
        for direction in (right, left):
            @pl.when(direction[0] == OUT - 1)
            def _():
                for s in range(1, OUT):
                    a_wait(direction, c, s)
        for j in range(1, INN):
            to = lax.rem(i + j, INN)
            span = pl.ds(pl.multiple_of(to * rows_w, rows_w), rows_w)
            g_send[c, j - 1] = jnp.dot(
                u_t[span, :], a_all[c], preferred_element_type=jnp.float32).astype(jnp.bfloat16)
            gx(c, j).start()
        span = pl.ds(pl.multiple_of(i * rows_w, rows_w), rows_w)
        wg_out[:, cols(c)] = jnp.dot(
            u_t[span, :], a_all[c], preferred_element_type=jnp.float32)

    load_qkv.wait()
    loop(heads, head)

    for j in range(1, OUT):
        uz(j).wait_recv()
        for k in range(1, XS):
            ux(j, k).start()
        uc(j, 0).start()
    for j in range(OUT):
        for k in range(1, XS):
            ux(j, k).wait_recv()
            uc(j, k).start()
    for j in range(OUT):
        for k in range(XS):
            uc(j, k).wait_recv()
    loop(OUT, flip)
    load_ow.wait()

    def tick(k):
        n = k + GROUP
        first = n - CHUNKS

        @pl.when((first >= 0) & (first < CHUNKS))
        def _():
            own_w(first).wait()
            for j in range(1, INN):
                wx(first, j).wait_recv()

        for direction in (right, left):
            a_item(direction, n)
            h_item(direction, n)

        @pl.when((first >= 0) & (first < CHUNKS))
        def _():
            hid_out[:, cols(first)] = partial(first, o)

        @pl.when(k < spans)
        def _():
            project(k)

        @pl.when(k == spans)
        def _():
            for j in range(1, TEN):
                att(j).start()

        m = n - 1 - DELAY - (OUT - 2) * GROUP
        turn = (OUT - 1) * GROUP
        rest = lax.rem(m, turn)

        @pl.when((m >= 0) & (rest < GROUP) & (m // turn * GROUP < CHUNKS))
        def _():
            weight_chunk(m // turn * GROUP + rest)

    loop(OUT * CHUNKS - GROUP, tick)

    total = part[pl.ds(pl.multiple_of(t * rows, rows), rows), :].astype(jnp.float32)
    total = total + bias[...].astype(jnp.float32)[None, :]
    for j in range(1, TEN):
        att(j).wait_recv()
        total = total + att_recv[j - 1].astype(jnp.float32)
    att_out[...] = total

    factor = 1.0 / (OUT * INN)

    for j in range(1, OUT):
        uz(j).wait_send()
    for j in range(OUT):
        for k in range(1, XS):
            ux(j, k).wait_send()
        for k in range(XS):
            uc(j, k).wait_send()
    for j in range(1, TEN):
        att(j).wait_send()

    def finish(c):
        acc = wg_out[:, cols(c)]
        for j in range(1, INN):
            gx(c, j).wait_recv()
            acc = acc + g_recv[c, j - 1].astype(jnp.float32)
        wg_out[:, cols(c)] = acc * factor
        for j in range(1, INN):
            wx(c, j).wait_send()
            gx(c, j).wait_send()
        for s in range(OUT - 1):
            @pl.when((o < OUT - 1) & (o >= s))
            def _():
                a_right(c, s).wait_send()

            @pl.when((o > 0) & (o + s <= OUT - 1))
            def _():
                a_left(c, s).wait_send()

    loop(CHUNKS, finish)

    def close(c):
        slope = gelu_slope(pre[:, cols(c)].astype(jnp.float32))

        @pl.when(o == 0)
        def _():
            h_l(c, o).wait_recv()
            hid_out[:, cols(c)] = (
                hid_out[:, cols(c)] + h_left[c, o].astype(jnp.float32)) * slope

        @pl.when(o == OUT - 1)
        def _():
            h_r(c, o).wait_recv()
            hid_out[:, cols(c)] = (
                hid_out[:, cols(c)] + h_right[c, o].astype(jnp.float32)) * slope

        @pl.when((o > 0) & (o < OUT - 1))
        def _():
            h_r(c, o).wait_recv()
            h_l(c, o).wait_recv()
            hid_out[:, cols(c)] = (
                hid_out[:, cols(c)] + h_right[c, o].astype(jnp.float32)
                + h_left[c, o].astype(jnp.float32)) * slope

        for s in range(OUT - 1):
            er, el = OUT - 1 - s, s

            @pl.when(o < er)
            def _():
                h_r(c, er).wait_send()

            @pl.when(o > el)
            def _():
                h_l(c, el).wait_send()

    loop(CHUNKS, close)


def write_out(att, hid, wg, att_hbm, hid_hbm, wg_hbm, sem):
    copies = []
    for n, (src, dst) in enumerate(((att, att_hbm), (hid, hid_hbm), (wg, wg_hbm))):
        step = src.shape[0] // PIECES
        for p in range(PIECES):
            span = pl.ds(p * step, step)
            copies.append(pltpu.make_async_copy(src.at[span, :], dst.at[span, :], sem.at[n, p]))
    for copy in copies:
        copy.start()
    for copy in copies:
        copy.wait()


def body(sizes, qkv, segment_ids, out_weight, out_bias, upstream, pre_act, down_weight):
    OUT, INN, TEN = sizes
    rows, width = upstream.shape
    tokens, ff = pre_act.shape
    rows_w = down_weight.shape[0]
    fc = ff // CHUNKS
    bf, f32 = jnp.bfloat16, jnp.float32
    vmem = pl.BlockSpec(memory_space=pltpu.VMEM)
    anym = pl.BlockSpec(memory_space=pl.ANY)
    dma = lambda *shape: pltpu.SemaphoreType.DMA(shape)
    block = min(tokens, 4 * ROWS_DEV)
    held = 4 * (rows * width + tokens * ff + rows_w * ff)
    attention_out, act_grad, weight_grad = pl.pallas_call(
        functools.partial(kernel, sizes),
        out_shape=(
            pltpu.VMEM((rows, width), f32),
            pltpu.VMEM((tokens, ff), f32),
            pltpu.VMEM((rows_w, ff), f32),
        ),
        in_specs=[anym] * 7,
        out_specs=(vmem, vmem, vmem),
        scratch_shapes=[
            pltpu.VMEM(segment_ids.shape, segment_ids.dtype),
            pltpu.VMEM(out_bias.shape, bf),
            pltpu.VMEM(qkv.shape, bf),
            pltpu.VMEM(out_weight.shape, bf),
            pltpu.VMEM((tokens, qkv.shape[2]), bf),
            pltpu.VMEM((tokens, width), bf),
            pltpu.VMEM((TEN - 1, rows, width), bf),
            pltpu.VMEM((rows, width), bf),
            pltpu.VMEM((OUT * tokens, INN * rows_w), bf),
            pltpu.VMEM((INN * rows_w, OUT * tokens), bf),
            pltpu.VMEM((CHUNKS, INN * rows_w, fc), bf),
            pltpu.VMEM((CHUNKS, OUT * tokens, fc), bf),
            pltpu.VMEM((tokens, ff), bf),
            pltpu.VMEM((tokens // block, block, block), f32),
            pltpu.VMEM((CHUNKS, OUT, tokens, fc), bf),
            pltpu.VMEM((CHUNKS, OUT, tokens, fc), bf),
            pltpu.VMEM((CHUNKS, INN - 1, rows_w, fc), bf),
            pltpu.VMEM((CHUNKS, INN - 1, rows_w, fc), bf),
            dma(6), dma(1, CHUNKS), dma(TEN - 1), dma(TEN - 1),
            dma(OUT - 1), dma(OUT - 1),
            dma(OUT, max(TEN // 2 - 1, 1)), dma(OUT, max(TEN // 2 - 1, 1)),
            dma(OUT, TEN // 2), dma(OUT, TEN // 2),
            dma(CHUNKS, INN - 1), dma(CHUNKS, INN - 1),
            dma(CHUNKS, OUT - 1), dma(CHUNKS, OUT - 1),
            dma(CHUNKS, OUT - 1), dma(CHUNKS, OUT - 1),
            dma(CHUNKS, OUT), dma(CHUNKS, OUT),
            dma(CHUNKS, OUT), dma(CHUNKS, OUT),
            dma(CHUNKS, INN - 1), dma(CHUNKS, INN - 1),
            pltpu.SemaphoreType.REGULAR((2,)),
        ],
        compiler_params=pltpu.CompilerParams(
            has_side_effects=True, collective_id=0, vmem_limit_bytes=64_000_000 - held),
        name="layer",
    )(qkv, segment_ids, out_weight, out_bias, upstream, pre_act, down_weight)
    results = tuple(
        pltpu.with_memory_space_constraint(r, pltpu.VMEM)
        for r in (attention_out, act_grad, weight_grad))
    return pl.pallas_call(
        write_out,
        out_shape=tuple(jax.ShapeDtypeStruct(r.shape, f32) for r in results),
        in_specs=[vmem] * 3,
        out_specs=(anym,) * 3,
        scratch_shapes=[dma(3, PIECES)],
        compiler_params=pltpu.CompilerParams(vmem_limit_bytes=2**20),
        name="write_out",
    )(*results)


def solution(mesh):
    dp, tensor = mesh.shape["dp"], mesh.shape["tensor"]
    inner = 2 ** ((dp.bit_length() - 1) // 2)
    return jax.shard_map(
        functools.partial(body, (dp // inner, inner, tensor)),
        mesh=mesh,
        in_specs=(
            P(None, "dp", "tensor"),
            P("dp", None, None),
            P(None, "tensor"),
            P(),
            P(("dp", "tensor"), None),
            P("dp", "tensor"),
            P("dp", "tensor"),
        ),
        out_specs=(P(("dp", "tensor"), None), P("dp", "tensor"), P("dp", "tensor")),
        check_vma=False,
    )
```

```python
import functools
import math

import jax
import jax.numpy as jnp
from jax import lax
from jax.experimental import pallas as pl
from jax.experimental.pallas import tpu as pltpu
from jax.sharding import PartitionSpec as P

HEAD = 128
ROWS_DEV = 64
CHUNKS = 4
GROUP = 2
DELAY = 1
PIECES = 4

root_half = 1.0 / math.sqrt(2.0)
inv_root_tau = 1.0 / math.sqrt(2.0 * math.pi)


def gelu_exact(argument):
    return 0.5 * argument * (1.0 + lax.erf(argument * root_half))


def gelu_slope(argument):
    return (
        0.5 * (1.0 + lax.erf(argument * root_half))
        + argument * jnp.exp(-0.5 * argument * argument) * inv_root_tau
    )


def kernel(
    sizes,
    qkv_hbm, names_hbm, ow_hbm, bias_hbm, up_hbm, pre_hbm, w_hbm,
    att_out, hid_out, wg_out,
    segments, bias, qkv, ow, ctx, part, att_recv,
    up, u_all, u_t, w_all, a_all, pre, same_ref, h_right, h_left, g_send, g_recv,
    local_sem, send_sem, z_r, uz_r, w_r, all_r, far_sem,
):
    OUT, INN, TEN = sizes
    XS = TEN // 2
    g = lax.axis_index("dp")
    t = lax.axis_index("tensor")
    o, i = g // INN, lax.rem(g, INN)
    x, core = t // 2, lax.rem(t, 2)
    rows_w, ff = w_hbm.shape
    rows = up_hbm.shape[0]
    tokens = rows * TEN
    fc = ff // CHUNKS
    dcols = rows_w * INN
    HOPS = OUT - 1

    def remote(src, dst, ssem, rsem, dp, tensor):
        return pltpu.make_async_remote_copy(
            src_ref=src, dst_ref=dst, send_sem=ssem, recv_sem=rsem,
            device_id={"dp": dp, "tensor": tensor},
            device_id_type=pl.DeviceIdType.MESH,
        )

    def cols(c):
        return pl.ds(pl.multiple_of(c * fc, fc), fc)

    def u_rows(oo, tt):
        return u_all.at[pl.ds(pl.multiple_of((oo * TEN + tt) * rows, rows), rows), :]

    def a_rows(c, oo):
        return a_all.at[c, pl.ds(pl.multiple_of(oo * tokens, tokens), tokens), :]

    def w_rows(c, ii):
        return w_all.at[c, pl.ds(pl.multiple_of(ii * rows_w, rows_w), rows_w), :]

    def uz(j):
        to = lax.rem(o + j, OUT)
        return remote(
            up.at[:, pl.ds(pl.multiple_of(to * dcols, dcols), dcols)],
            u_rows(o, t), send_sem.at[2], uz_r.at[j - 1], to * INN + i, t,
        )

    def ux(j, k):
        block = u_rows(lax.rem(o - j + OUT, OUT), t)
        return remote(block, block, send_sem.at[3], all_r.at[0], g,
                      lax.rem(x + k, XS) * 2 + core)

    def uc(j, k):
        block = u_rows(lax.rem(o - j + OUT, OUT), lax.rem(x - k + XS, XS) * 2 + core)
        return remote(block, block, send_sem.at[4], all_r.at[1], g, x * 2 + 1 - core)

    def wx(c, j):
        return remote(w_hbm.at[:, cols(c)], w_rows(c, i), send_sem.at[5], w_r.at[c],
                      o * INN + lax.rem(i + j, INN), t)

    def a_right(c, s, n):
        block = a_rows(c, jnp.maximum(o - s, 0))
        return remote(block, block, send_sem.at[0], z_r.at[0, n],
                      jnp.minimum(o + 1, OUT - 1) * INN + i, t)

    def a_left(c, s, n):
        block = a_rows(c, jnp.minimum(o + s, OUT - 1))
        return remote(block, block, send_sem.at[1], z_r.at[1, n],
                      jnp.maximum(o - 1, 0) * INN + i, t)

    def h_r(c, e, n):
        return remote(h_right.at[c, e], h_right.at[c, e], send_sem.at[0], z_r.at[0, n],
                      jnp.minimum(o + 1, OUT - 1) * INN + i, t)

    def h_l(c, e, n):
        return remote(h_left.at[c, e], h_left.at[c, e], send_sem.at[1], z_r.at[1, n],
                      jnp.maximum(o - 1, 0) * INN + i, t)

    def gx(c, j):
        return remote(g_send.at[c, j - 1], g_recv.at[c, j - 1], send_sem.at[6], all_r.at[3],
                      o * INN + lax.rem(i + j, INN), t)

    def att(j):
        to = lax.rem(t + j, TEN)
        return remote(part.at[pl.ds(pl.multiple_of(to * rows, rows), rows), :],
                      att_recv.at[j - 1], send_sem.at[7], all_r.at[2], g, to)

    def own_w(c):
        return pltpu.make_async_copy(w_hbm.at[:, cols(c)], w_rows(c, i), local_sem.at[6])

    def sent(ref, stream):
        remote(ref, ref, send_sem.at[stream], send_sem.at[stream], g, t).wait_send()

    def landed(ref, semaphore):
        remote(ref, ref, semaphore, semaphore, g, t).wait_recv()

    def loop(count, fn):
        def step(index, carry):
            fn(index)
            return carry
        lax.fori_loop(0, count, step, 0)

    load_up = pltpu.make_async_copy(up_hbm, up, local_sem.at[0])
    near = sorted({1, OUT - 1})
    far = list(range(2, OUT - 1))
    load_qkv = pltpu.make_async_copy(qkv_hbm, qkv, local_sem.at[1])
    load_ow = pltpu.make_async_copy(ow_hbm, ow, local_sem.at[2])
    load_pre = pltpu.make_async_copy(pre_hbm, pre, local_sem.at[3])

    load_names = pltpu.make_async_copy(names_hbm, segments, local_sem.at[4])
    load_bias = pltpu.make_async_copy(bias_hbm, bias, local_sem.at[5])

    def signal(semaphore, dp, tensor):
        pl.semaphore_signal(semaphore, inc=1, device_id={"dp": dp, "tensor": tensor},
                            device_id_type=pl.DeviceIdType.MESH)

    load_up.start()
    load_pre.start()
    partners = (
        [(o * INN + lax.rem(i + j, INN), t) for j in range(1, INN)]
        + [(g, lax.rem(t + j, TEN)) for j in range(1, TEN)])
    barrier = pltpu.get_barrier_semaphore()

    @pl.when(o < OUT - 1)
    def _():
        signal(barrier, jnp.minimum(o + 1, OUT - 1) * INN + i, t)

    @pl.when(o > 0)
    def _():
        signal(barrier, jnp.maximum(o - 1, 0) * INN + i, t)

    for dp, tensor in partners:
        signal(barrier, dp, tensor)
    load_up.wait()
    sides = jnp.minimum(o, 1) + jnp.minimum(OUT - 1 - o, 1)
    pl.semaphore_wait(barrier, len(partners) + sides)

    def uz_near(to):
        return (to - o == 1) | (o - to == 1)

    for j in near:
        @pl.when(uz_near(lax.rem(o + j, OUT)))
        def _():
            uz(j).start()
    def start_w(c):
        for j in range(1, INN):
            wx(c, j).start()
        own_w(c).start()

    if OUT > 2:
        @pl.when(o >= 2)
        def _():
            pl.semaphore_wait(far_sem.at[0], 1)

        @pl.when((o >= 1) & (o <= OUT - 2))
        def _():
            signal(far_sem.at[0], jnp.minimum(o + 1, OUT - 1) * INN + i, t)

        loop(CHUNKS, start_w)

        @pl.when(o <= OUT - 3)
        def _():
            pl.semaphore_wait(far_sem.at[1], 1)

        @pl.when((o >= 1) & (o <= OUT - 2))
        def _():
            signal(far_sem.at[1], jnp.maximum(o - 1, 0) * INN + i, t)
    else:
        loop(CHUNKS, start_w)
    for j in range(1, OUT):
        @pl.when(jnp.logical_not(uz_near(lax.rem(o + j, OUT))))
        def _():
            uz(j).start()
    load_names.start()
    load_bias.start()
    load_qkv.start()
    load_ow.start()
    u_all[pl.ds(pl.multiple_of((o * TEN + t) * rows, rows), rows), :] = (
        up[:, pl.ds(pl.multiple_of(o * dcols, dcols), dcols)])

    right = (o, lambda p: p, a_right, z_r.at[0], h_right, h_r)
    left = (OUT - 1 - o, lambda p: OUT - 1 - p, a_left, z_r.at[1], h_left, h_l)

    def a_wait(direction, c, s):
        r, place, _, arrived, _, _ = direction
        step = c // GROUP * GROUP * r + (s - 1) * GROUP + lax.rem(c, GROUP)
        landed(a_rows(c, place(jnp.maximum(r - s, 0))), arrived.at[step])

    def a_item(direction, n):
        r, _, copy, _, _, _ = direction
        turn = (r + 1) * GROUP
        rest = lax.rem(n, turn)
        s = rest // GROUP
        c = n // turn * GROUP + lax.rem(rest, GROUP)

        @pl.when((r < OUT - 1) & (n < (r + 1) * CHUNKS))
        def _():
            @pl.when(s > 0)
            def _():
                a_wait(direction, c, s)
            copy(c, s, n).start()

    def activate(c):
        act = gelu_exact(pre[:, cols(c)].astype(jnp.float32)).astype(jnp.bfloat16)
        a_all[c, pl.ds(pl.multiple_of(o * tokens, tokens), tokens), :] = act

    def open_group(n):
        activate(n)
        a_item(right, n)
        a_item(left, n)

    load_pre.wait()
    loop(GROUP, open_group)
    for k in range(1, XS):
        ux(0, k).start()
    uc(0, 0).start()
    loop(CHUNKS - GROUP, lambda n: activate(n + GROUP))

    heads = qkv.shape[2] // HEAD
    block = min(tokens, 4 * ROWS_DEV)
    scale = 1.0 / math.sqrt(HEAD)

    load_names.wait()
    load_bias.wait()
    labels = segments[0].astype(jnp.float32)
    packs, length = labels.shape
    spread = (
        lax.rem(lax.broadcasted_iota(jnp.int32, (length, tokens), 1), length)
        == lax.broadcasted_iota(jnp.int32, (length, tokens), 0)
    ).astype(jnp.float32)
    wide = jnp.dot(labels, spread, preferred_element_type=jnp.float32)
    pack = lax.broadcasted_iota(jnp.int32, (packs, tokens), 0)
    here = lax.broadcasted_iota(jnp.int32, (packs, tokens), 1) // length == pack
    name = jnp.sum(
        jnp.where(here, wide + 2.0 * pack.astype(jnp.float32), 0.0), axis=0, keepdims=True)
    for b in range(tokens // block):
        across = jnp.broadcast_to(name[:, b * block : (b + 1) * block], (block, block))
        same_ref[b] = (across == across.T).astype(jnp.float32)

    def head(h):
        lanes = pl.ds(pl.multiple_of(h * HEAD, HEAD), HEAD)
        for b in range(tokens // block):
            mine = slice(b * block, (b + 1) * block)
            same = same_ref[b] > 0.5
            scores = lax.dot_general(
                qkv[0, mine, lanes], qkv[1, mine, lanes], (((1,), (1,)), ((), ())),
                preferred_element_type=jnp.float32) * scale
            masked = jnp.where(same, scores, -1e30)
            top = jnp.max(masked, axis=1, keepdims=True)
            exponent = jnp.where(same, jnp.exp(masked - top), 0.0)
            weights = (exponent / jnp.sum(exponent, axis=1, keepdims=True)).astype(jnp.bfloat16)
            ctx[mine, lanes] = jnp.dot(
                weights, qkv[2, mine, lanes], preferred_element_type=jnp.float32
            ).astype(jnp.bfloat16)

    nb = 512
    spans = ow.shape[0] // nb

    def project(n):
        span = pl.ds(pl.multiple_of(n * nb, nb), nb)
        part[:, span] = lax.dot_general(
            ctx[...], ow[span, :], (((1,), (1,)), ((), ())),
            preferred_element_type=jnp.float32).astype(jnp.bfloat16)

    def flip(e):
        span = pl.ds(pl.multiple_of(e * tokens, tokens), tokens)
        u_t[:, span] = u_all[span, :].T

    def partial(c, e):
        span = pl.ds(pl.multiple_of(e * tokens, tokens), tokens)
        return jnp.dot(u_all[span, :], w_all[c], preferred_element_type=jnp.float32)

    def h_item(direction, n):
        r, place, _, arrived, held, copy = direction
        m = n - (r + 1) * CHUNKS
        e = place(OUT - 1 - m // CHUNKS)
        c = lax.rem(m, CHUNKS)

        @pl.when((m >= 0) & (r == 0))
        def _():
            held[c, e] = partial(c, e).astype(jnp.bfloat16)
            copy(c, e, n).start()

        @pl.when((m >= 0) & (r > 0) & (r < OUT - 1))
        def _():
            mine = partial(c, e)
            landed(held.at[c, e], arrived.at[n - CHUNKS])
            held[c, e] = (mine + held[c, e].astype(jnp.float32)).astype(jnp.bfloat16)
            copy(c, e, n).start()

    def weight_chunk(c):
        for direction in (right, left):
            @pl.when(direction[0] == OUT - 1)
            def _():
                for s in range(1, OUT):
                    a_wait(direction, c, s)
        for j in range(1, INN):
            to = lax.rem(i + j, INN)
            span = pl.ds(pl.multiple_of(to * rows_w, rows_w), rows_w)
            g_send[c, j - 1] = jnp.dot(
                u_t[span, :], a_all[c], preferred_element_type=jnp.float32).astype(jnp.bfloat16)
            gx(c, j).start()
        span = pl.ds(pl.multiple_of(i * rows_w, rows_w), rows_w)
        wg_out[:, cols(c)] = jnp.dot(
            u_t[span, :], a_all[c], preferred_element_type=jnp.float32)

    load_qkv.wait()
    loop(heads, head)

    for j in range(1, OUT):
        uz(j).wait_recv()
        for k in range(1, XS):
            ux(j, k).start()
        uc(j, 0).start()
    load_ow.wait()
    early = spans // 2
    loop(early, project)

    def relay(n):
        a_item(right, n)
        a_item(left, n)

    loop(CHUNKS - GROUP - 1, lambda n: relay(n + GROUP))
    if XS > 1:
        landed(u_all.at[pl.ds(0, OUT * (XS - 1) * rows), :], all_r.at[0])
    for j in range(OUT):
        for k in range(1, XS):
            uc(j, k).start()
    relay(CHUNKS - 1)
    landed(u_all.at[pl.ds(0, OUT * XS * rows), :], all_r.at[1])
    loop(OUT, flip)
    own_rows = g_send.at[:, 0]
    pltpu.make_async_copy(own_rows, own_rows, local_sem.at[6]).wait()
    lead = max(DELAY, CHUNKS - 1 - (OUT - 2) * GROUP) + 1 + (OUT - 2) * GROUP

    def tick(k):
        n = k + CHUNKS
        first = k

        @pl.when(first < CHUNKS)
        def _():
            landed(g_recv.at[first], w_r.at[first])

        for direction in (right, left):
            a_item(direction, n)
            h_item(direction, n)

        @pl.when(first < CHUNKS)
        def _():
            hid_out[:, cols(first)] = partial(first, o)

        @pl.when(k < spans - early)
        def _():
            project(k + early)

        @pl.when(k == spans - early)
        def _():
            for j in range(1, TEN):
                att(j).start()

        m = n - lead
        turn = (OUT - 1) * GROUP
        rest = lax.rem(m, turn)

        @pl.when((m >= 0) & (rest < GROUP) & (m // turn * GROUP < CHUNKS))
        def _():
            weight_chunk(m // turn * GROUP + rest)

    loop((OUT - 1) * CHUNKS, tick)

    total = part[pl.ds(pl.multiple_of(t * rows, rows), rows), :].astype(jnp.float32)
    total = total + bias[...].astype(jnp.float32)[None, :]
    landed(att_recv, all_r.at[2])
    for j in range(1, TEN):
        total = total + att_recv[j - 1].astype(jnp.float32)
    att_out[...] = total

    factor = 1.0 / (OUT * INN)

    landed(g_recv, all_r.at[3])

    def finish(c):
        acc = wg_out[:, cols(c)]
        for j in range(1, INN):
            acc = acc + g_recv[c, j - 1].astype(jnp.float32)
        wg_out[:, cols(c)] = acc * factor

    loop(CHUNKS, finish)
    sent(up.at[:, pl.ds(0, (OUT - 1) * dcols)], 2)
    if XS > 1:
        sent(u_all.at[pl.ds(0, OUT * (XS - 1) * rows), :], 3)
    sent(u_all.at[pl.ds(0, OUT * XS * rows), :], 4)
    sent(g_send, 5)
    sent(g_send, 6)
    sent(att_recv, 7)
    final = (OUT - 1) * CHUNKS

    def close(c):
        slope = gelu_slope(pre[:, cols(c)].astype(jnp.float32))

        @pl.when(o == 0)
        def _():
            landed(h_left.at[c, o], z_r.at[1, final + c])
            hid_out[:, cols(c)] = (
                hid_out[:, cols(c)] + h_left[c, o].astype(jnp.float32)) * slope

        @pl.when(o == OUT - 1)
        def _():
            landed(h_right.at[c, o], z_r.at[0, final + c])
            hid_out[:, cols(c)] = (
                hid_out[:, cols(c)] + h_right[c, o].astype(jnp.float32)) * slope

        @pl.when((o > 0) & (o < OUT - 1))
        def _():
            landed(h_right.at[c, o], z_r.at[0, final + c])
            landed(h_left.at[c, o], z_r.at[1, final + c])
            hid_out[:, cols(c)] = (
                hid_out[:, cols(c)] + h_right[c, o].astype(jnp.float32)
                + h_left[c, o].astype(jnp.float32)) * slope

    loop(CHUNKS, close)

    @pl.when(o < OUT - 1)
    def _():
        sent(a_all, 0)

    @pl.when(o > 0)
    def _():
        sent(a_all, 1)


def write_out(att, hid, wg, att_hbm, hid_hbm, wg_hbm, sem):
    pairs = ((att, att_hbm), (hid, hid_hbm), (wg, wg_hbm))
    for n, (src, dst) in enumerate(pairs):
        step = src.shape[0] // PIECES
        for p in range(PIECES):
            span = pl.ds(p * step, step)
            pltpu.make_async_copy(src.at[span, :], dst.at[span, :], sem.at[n]).start()
    for n, (src, dst) in enumerate(pairs):
        pltpu.make_async_copy(src, dst, sem.at[n]).wait()


def body(sizes, qkv, segment_ids, out_weight, out_bias, upstream, pre_act, down_weight):
    OUT, INN, TEN = sizes
    rows, width = upstream.shape
    tokens, ff = pre_act.shape
    rows_w = down_weight.shape[0]
    fc = ff // CHUNKS
    bf, f32 = jnp.bfloat16, jnp.float32
    vmem = pl.BlockSpec(memory_space=pltpu.VMEM)
    anym = pl.BlockSpec(memory_space=pl.ANY)
    dma = lambda *shape: pltpu.SemaphoreType.DMA(shape)
    block = min(tokens, 4 * ROWS_DEV)
    held = 4 * (rows * width + tokens * ff + rows_w * ff)
    attention_out, act_grad, weight_grad = pl.pallas_call(
        functools.partial(kernel, sizes),
        out_shape=(
            pltpu.VMEM((rows, width), f32),
            pltpu.VMEM((tokens, ff), f32),
            pltpu.VMEM((rows_w, ff), f32),
        ),
        in_specs=[anym] * 7,
        out_specs=(vmem, vmem, vmem),
        scratch_shapes=[
            pltpu.VMEM(segment_ids.shape, segment_ids.dtype),
            pltpu.VMEM(out_bias.shape, bf),
            pltpu.VMEM(qkv.shape, bf),
            pltpu.VMEM(out_weight.shape, bf),
            pltpu.VMEM((tokens, qkv.shape[2]), bf),
            pltpu.VMEM((tokens, width), bf),
            pltpu.VMEM((TEN - 1, rows, width), bf),
            pltpu.VMEM((rows, width), bf),
            pltpu.VMEM((OUT * tokens, INN * rows_w), bf),
            pltpu.VMEM((INN * rows_w, OUT * tokens), bf),
            pltpu.VMEM((CHUNKS, INN * rows_w, fc), bf),
            pltpu.VMEM((CHUNKS, OUT * tokens, fc), bf),
            pltpu.VMEM((tokens, ff), bf),
            pltpu.VMEM((tokens // block, block, block), f32),
            pltpu.VMEM((CHUNKS, OUT, tokens, fc), bf),
            pltpu.VMEM((CHUNKS, OUT, tokens, fc), bf),
            pltpu.VMEM((CHUNKS, INN - 1, rows_w, fc), bf),
            pltpu.VMEM((CHUNKS, INN - 1, rows_w, fc), bf),
            dma(7), dma(8), dma(2, OUT * CHUNKS), dma(OUT - 1), dma(CHUNKS), dma(4),
            pltpu.SemaphoreType.REGULAR((2,)),
        ],
        compiler_params=pltpu.CompilerParams(
            has_side_effects=True, collective_id=0, vmem_limit_bytes=64_000_000 - held),
        name="layer",
    )(qkv, segment_ids, out_weight, out_bias, upstream, pre_act, down_weight)
    results = tuple(
        pltpu.with_memory_space_constraint(r, pltpu.VMEM)
        for r in (attention_out, act_grad, weight_grad))
    return pl.pallas_call(
        write_out,
        out_shape=tuple(jax.ShapeDtypeStruct(r.shape, f32) for r in results),
        in_specs=[vmem] * 3,
        out_specs=(anym,) * 3,
        scratch_shapes=[dma(3)],
        compiler_params=pltpu.CompilerParams(vmem_limit_bytes=2**20),
        name="write_out",
    )(*results)


def solution(mesh):
    dp, tensor = mesh.shape["dp"], mesh.shape["tensor"]
    inner = 2 ** ((dp.bit_length() - 1) // 2)
    return jax.shard_map(
        functools.partial(body, (dp // inner, inner, tensor)),
        mesh=mesh,
        in_specs=(
            P(None, "dp", "tensor"),
            P("dp", None, None),
            P(None, "tensor"),
            P(),
            P(("dp", "tensor"), None),
            P("dp", "tensor"),
            P("dp", "tensor"),
        ),
        out_specs=(P(("dp", "tensor"), None), P("dp", "tensor"), P("dp", "tensor")),
        check_vma=False,
    )
```

```python
import functools
import math

import jax
import jax.numpy as jnp
from jax import lax
from jax.experimental import pallas as pl
from jax.experimental.pallas import tpu as pltpu
from jax.sharding import PartitionSpec as P

HEAD = 128
ROWS_DEV = 64
CHUNKS = 4
GROUP = 2
DELAY = 1
PIECES = 4

root_half = 1.0 / math.sqrt(2.0)
inv_root_tau = 1.0 / math.sqrt(2.0 * math.pi)


def gelu_exact(argument):
    return 0.5 * argument * (1.0 + lax.erf(argument * root_half))


def gelu_slope(argument):
    return (
        0.5 * (1.0 + lax.erf(argument * root_half))
        + argument * jnp.exp(-0.5 * argument * argument) * inv_root_tau
    )


def kernel(
    sizes,
    qkv_hbm, names_hbm, ow_hbm, bias_hbm, up_hbm, pre_hbm, w_hbm,
    att_out, hid_out, wg_out,
    segments, bias, qkv, ow, ctx, part, att_recv,
    up, u_all, u_t, w_all, a_all, pre, same_ref, h_right, h_left, g_send, g_recv,
    local_sem, send_sem, z_r, uz_r, w_r, all_r, far_sem,
):
    OUT, INN, TEN = sizes
    XS = TEN // 2
    g = lax.axis_index("dp")
    t = lax.axis_index("tensor")
    o, i = g // INN, lax.rem(g, INN)
    x, core = t // 2, lax.rem(t, 2)
    rows_w, ff = w_hbm.shape
    rows = up_hbm.shape[0]
    tokens = rows * TEN
    fc = ff // CHUNKS
    dcols = rows_w * INN
    HOPS = OUT - 1

    def remote(src, dst, ssem, rsem, dp, tensor):
        return pltpu.make_async_remote_copy(
            src_ref=src, dst_ref=dst, send_sem=ssem, recv_sem=rsem,
            device_id={"dp": dp, "tensor": tensor},
            device_id_type=pl.DeviceIdType.MESH,
        )

    def cols(c):
        return pl.ds(pl.multiple_of(c * fc, fc), fc)

    def u_rows(oo, tt):
        return u_all.at[pl.ds(pl.multiple_of((oo * TEN + tt) * rows, rows), rows), :]

    def a_rows(c, oo):
        return a_all.at[c, pl.ds(pl.multiple_of(oo * tokens, tokens), tokens), :]

    def w_rows(c, ii):
        return w_all.at[c, pl.ds(pl.multiple_of(ii * rows_w, rows_w), rows_w), :]

    def uz(j):
        to = lax.rem(o + j, OUT)
        return remote(
            up.at[:, pl.ds(pl.multiple_of(to * dcols, dcols), dcols)],
            u_rows(o, t), send_sem.at[2], uz_r.at[j - 1], to * INN + i, t,
        )

    def ux(j, k):
        block = u_rows(lax.rem(o - j + OUT, OUT), t)
        return remote(block, block, send_sem.at[2], all_r.at[0], g,
                      lax.rem(x + k, XS) * 2 + core)

    def uc(j, k):
        block = u_rows(lax.rem(o - j + OUT, OUT), lax.rem(x - k + XS, XS) * 2 + core)
        return remote(block, block, send_sem.at[2], all_r.at[1], g, x * 2 + 1 - core)

    def wx(c, j):
        return remote(w_hbm.at[:, cols(c)], w_rows(c, i), send_sem.at[3], w_r.at[c],
                      o * INN + lax.rem(i + j, INN), t)

    def a_right(c, s, n):
        block = a_rows(c, jnp.maximum(o - s, 0))
        return remote(block, block, send_sem.at[0], z_r.at[n],
                      jnp.minimum(o + 1, OUT - 1) * INN + i, t)

    def a_left(c, s, n):
        block = a_rows(c, jnp.minimum(o + s, OUT - 1))
        return remote(block, block, send_sem.at[1], z_r.at[n],
                      jnp.maximum(o - 1, 0) * INN + i, t)

    def h_r(c, e, n):
        return remote(h_right.at[c, e], h_right.at[c, e], send_sem.at[0], z_r.at[n],
                      jnp.minimum(o + 1, OUT - 1) * INN + i, t)

    def h_l(c, e, n):
        return remote(h_left.at[c, e], h_left.at[c, e], send_sem.at[1], z_r.at[n],
                      jnp.maximum(o - 1, 0) * INN + i, t)

    def gx(c, j):
        return remote(g_send.at[c, j - 1], g_recv.at[c, j - 1], send_sem.at[4], all_r.at[3],
                      o * INN + lax.rem(i + j, INN), t)

    def att(j):
        to = lax.rem(t + j, TEN)
        return remote(part.at[pl.ds(pl.multiple_of(to * rows, rows), rows), :],
                      att_recv.at[j - 1], send_sem.at[5], all_r.at[2], g, to)

    def own_w(c):
        return pltpu.make_async_copy(w_hbm.at[:, cols(c)], w_rows(c, i), local_sem.at[6])

    def sent(ref, stream):
        remote(ref, ref, send_sem.at[stream], send_sem.at[stream], g, t).wait_send()

    def landed(ref, semaphore):
        remote(ref, ref, semaphore, semaphore, g, t).wait_recv()

    def loop(count, fn):
        def step(index, carry):
            fn(index)
            return carry
        lax.fori_loop(0, count, step, 0)

    load_up = pltpu.make_async_copy(up_hbm, up, local_sem.at[0])
    near = sorted({1, OUT - 1})
    far = list(range(2, OUT - 1))
    load_qkv = pltpu.make_async_copy(qkv_hbm, qkv, local_sem.at[1])
    load_ow = pltpu.make_async_copy(ow_hbm, ow, local_sem.at[2])
    load_pre = pltpu.make_async_copy(pre_hbm, pre, local_sem.at[3])

    load_names = pltpu.make_async_copy(names_hbm, segments, local_sem.at[4])
    load_bias = pltpu.make_async_copy(bias_hbm, bias, local_sem.at[5])

    def signal(semaphore, dp, tensor):
        pl.semaphore_signal(semaphore, inc=1, device_id={"dp": dp, "tensor": tensor},
                            device_id_type=pl.DeviceIdType.MESH)

    load_up.start()
    load_pre.start()
    partners = (
        [(o * INN + lax.rem(i + j, INN), t) for j in range(1, INN)]
        + [(g, lax.rem(t + j, TEN)) for j in range(1, TEN)])
    barrier = pltpu.get_barrier_semaphore()

    @pl.when(o < OUT - 1)
    def _():
        signal(barrier, jnp.minimum(o + 1, OUT - 1) * INN + i, t)

    @pl.when(o > 0)
    def _():
        signal(barrier, jnp.maximum(o - 1, 0) * INN + i, t)

    for dp, tensor in partners:
        signal(barrier, dp, tensor)
    load_up.wait()
    sides = jnp.minimum(o, 1) + jnp.minimum(OUT - 1 - o, 1)
    pl.semaphore_wait(barrier, len(partners) + sides)

    def uz_near(to):
        return (to - o == 1) | (o - to == 1)

    for j in near:
        @pl.when(uz_near(lax.rem(o + j, OUT)))
        def _():
            uz(j).start()
    def start_w(c):
        for j in range(1, INN):
            wx(c, j).start()
        own_w(c).start()

    if OUT > 2:
        @pl.when(o >= 2)
        def _():
            pl.semaphore_wait(far_sem.at[0], 1)

        @pl.when((o >= 1) & (o <= OUT - 2))
        def _():
            signal(far_sem.at[0], jnp.minimum(o + 1, OUT - 1) * INN + i, t)

        loop(CHUNKS, start_w)

        @pl.when(o <= OUT - 3)
        def _():
            pl.semaphore_wait(far_sem.at[1], 1)

        @pl.when((o >= 1) & (o <= OUT - 2))
        def _():
            signal(far_sem.at[1], jnp.maximum(o - 1, 0) * INN + i, t)
    else:
        loop(CHUNKS, start_w)
    for j in range(1, OUT):
        @pl.when(jnp.logical_not(uz_near(lax.rem(o + j, OUT))))
        def _():
            uz(j).start()
    load_names.start()
    load_bias.start()
    load_qkv.start()
    load_ow.start()
    u_all[pl.ds(pl.multiple_of((o * TEN + t) * rows, rows), rows), :] = (
        up[:, pl.ds(pl.multiple_of(o * dcols, dcols), dcols)])

    right = (o, lambda p: p, a_right, h_right, h_r)
    left = (OUT - 1 - o, lambda p: OUT - 1 - p, a_left, h_left, h_l)
    steps = OUT * CHUNKS

    def items(count):
        return a_all.at[0, pl.ds(0, count * tokens), :]

    def relayed(n):
        used = 0
        for r in (o, OUT - 1 - o):
            own = (n < (r + 1) * CHUNKS) & (lax.rem(n, (r + 1) * GROUP) < GROUP)
            used = used + jnp.where((r > 0) & (r < OUT - 1) & jnp.logical_not(own), 1, 0)
        for count in (1, 2):
            @pl.when(used == count)
            def _():
                landed(items(count), z_r.at[n])

    def a_item(direction, n):
        r, _, copy, _, _ = direction
        turn = (r + 1) * GROUP
        rest = lax.rem(n, turn)
        s = rest // GROUP
        c = n // turn * GROUP + lax.rem(rest, GROUP)

        @pl.when((r < OUT - 1) & (n < (r + 1) * CHUNKS))
        def _():
            later = n + (n // turn + 1) * GROUP
            copy(c, s, jnp.where(r == OUT - 2, c, later)).start()

    def activate(c):
        act = gelu_exact(pre[:, cols(c)].astype(jnp.float32)).astype(jnp.bfloat16)
        a_all[c, pl.ds(pl.multiple_of(o * tokens, tokens), tokens), :] = act

    def open_group(n):
        activate(n)
        a_item(right, n)
        a_item(left, n)

    load_pre.wait()
    loop(GROUP, open_group)
    for k in range(1, XS):
        ux(0, k).start()
    uc(0, 0).start()
    loop(CHUNKS - GROUP, lambda n: activate(n + GROUP))

    heads = qkv.shape[2] // HEAD
    block = min(tokens, 4 * ROWS_DEV)
    scale = 1.0 / math.sqrt(HEAD)

    load_names.wait()
    load_bias.wait()
    labels = segments[0].astype(jnp.float32)
    packs, length = labels.shape
    spread = (
        lax.rem(lax.broadcasted_iota(jnp.int32, (length, tokens), 1), length)
        == lax.broadcasted_iota(jnp.int32, (length, tokens), 0)
    ).astype(jnp.float32)
    wide = jnp.dot(labels, spread, preferred_element_type=jnp.float32)
    pack = lax.broadcasted_iota(jnp.int32, (packs, tokens), 0)
    here = lax.broadcasted_iota(jnp.int32, (packs, tokens), 1) // length == pack
    name = jnp.sum(
        jnp.where(here, wide + 2.0 * pack.astype(jnp.float32), 0.0), axis=0, keepdims=True)
    for b in range(tokens // block):
        across = jnp.broadcast_to(name[:, b * block : (b + 1) * block], (block, block))
        same_ref[b] = (across == across.T).astype(jnp.float32)

    def head(h):
        lanes = pl.ds(pl.multiple_of(h * HEAD, HEAD), HEAD)
        for b in range(tokens // block):
            mine = slice(b * block, (b + 1) * block)
            same = same_ref[b] > 0.5
            scores = lax.dot_general(
                qkv[0, mine, lanes], qkv[1, mine, lanes], (((1,), (1,)), ((), ())),
                preferred_element_type=jnp.float32) * scale
            masked = jnp.where(same, scores, -1e30)
            top = jnp.max(masked, axis=1, keepdims=True)
            exponent = jnp.where(same, jnp.exp(masked - top), 0.0)
            weights = (exponent / jnp.sum(exponent, axis=1, keepdims=True)).astype(jnp.bfloat16)
            ctx[mine, lanes] = jnp.dot(
                weights, qkv[2, mine, lanes], preferred_element_type=jnp.float32
            ).astype(jnp.bfloat16)

    nb = 512
    spans = ow.shape[0] // nb

    def project(n):
        span = pl.ds(pl.multiple_of(n * nb, nb), nb)
        part[:, span] = lax.dot_general(
            ctx[...], ow[span, :], (((1,), (1,)), ((), ())),
            preferred_element_type=jnp.float32).astype(jnp.bfloat16)

    def flip(e):
        span = pl.ds(pl.multiple_of(e * tokens, tokens), tokens)
        u_t[:, span] = u_all[span, :].T

    def partial(c, e):
        span = pl.ds(pl.multiple_of(e * tokens, tokens), tokens)
        return jnp.dot(u_all[span, :], w_all[c], preferred_element_type=jnp.float32)

    def h_item(direction, n):
        r, place, _, held, copy = direction
        m = n - (r + 1) * CHUNKS
        e = place(OUT - 1 - m // CHUNKS)
        c = lax.rem(m, CHUNKS)
        slot = n + CHUNKS

        @pl.when((m >= 0) & (r == 0))
        def _():
            held[c, e] = partial(c, e).astype(jnp.bfloat16)
            copy(c, e, slot).start()

        @pl.when((m >= 0) & (r > 0) & (r < OUT - 1))
        def _():
            mine = partial(c, e)
            held[c, e] = (mine + held[c, e].astype(jnp.float32)).astype(jnp.bfloat16)
            copy(c, e, slot).start()

    def weight_chunk(c):
        for direction in (right, left):
            @pl.when(direction[0] == OUT - 1)
            def _():
                landed(items(OUT - 1), z_r.at[c])
        for j in range(1, INN):
            to = lax.rem(i + j, INN)
            span = pl.ds(pl.multiple_of(to * rows_w, rows_w), rows_w)
            g_send[c, j - 1] = jnp.dot(
                u_t[span, :], a_all[c], preferred_element_type=jnp.float32).astype(jnp.bfloat16)
            gx(c, j).start()
        span = pl.ds(pl.multiple_of(i * rows_w, rows_w), rows_w)
        wg_out[:, cols(c)] = jnp.dot(
            u_t[span, :], a_all[c], preferred_element_type=jnp.float32)

    load_qkv.wait()
    loop(heads, head)

    for j in range(1, OUT):
        uz(j).wait_recv()
        for k in range(1, XS):
            ux(j, k).start()
        uc(j, 0).start()
    load_ow.wait()
    early = spans // 2
    loop(early, project)

    def relay(n):
        relayed(n)
        a_item(right, n)
        a_item(left, n)

    loop(CHUNKS - GROUP - 1, lambda n: relay(n + GROUP))
    if XS > 1:
        landed(u_all.at[pl.ds(0, OUT * (XS - 1) * rows), :], all_r.at[0])
    for j in range(OUT):
        for k in range(1, XS):
            uc(j, k).start()
    relay(CHUNKS - 1)
    landed(u_all.at[pl.ds(0, OUT * XS * rows), :], all_r.at[1])
    loop(OUT, flip)
    own_rows = g_send.at[:, 0]
    pltpu.make_async_copy(own_rows, own_rows, local_sem.at[6]).wait()
    lead = max(DELAY, CHUNKS - 1 - (OUT - 2) * GROUP) + 1 + (OUT - 2) * GROUP

    def tick(k):
        n = k + CHUNKS
        first = k

        @pl.when(first < CHUNKS)
        def _():
            landed(g_recv.at[first], w_r.at[first])

        relayed(n)
        for direction in (right, left):
            a_item(direction, n)
            h_item(direction, n)

        @pl.when(first < CHUNKS)
        def _():
            hid_out[:, cols(first)] = partial(first, o)

        @pl.when(k < spans - early)
        def _():
            project(k + early)

        @pl.when(k == spans - early)
        def _():
            for j in range(1, TEN):
                att(j).start()

        m = n - lead
        turn = (OUT - 1) * GROUP
        rest = lax.rem(m, turn)

        @pl.when((m >= 0) & (rest < GROUP) & (m // turn * GROUP < CHUNKS))
        def _():
            weight_chunk(m // turn * GROUP + rest)

    loop((OUT - 1) * CHUNKS, tick)

    total = part[pl.ds(pl.multiple_of(t * rows, rows), rows), :].astype(jnp.float32)
    total = total + bias[...].astype(jnp.float32)[None, :]
    landed(att_recv, all_r.at[2])
    for j in range(1, TEN):
        total = total + att_recv[j - 1].astype(jnp.float32)
    att_out[...] = total

    factor = 1.0 / (OUT * INN)

    landed(g_recv, all_r.at[3])

    def finish(c):
        acc = wg_out[:, cols(c)]
        for j in range(1, INN):
            acc = acc + g_recv[c, j - 1].astype(jnp.float32)
        wg_out[:, cols(c)] = acc * factor

    loop(CHUNKS, finish)
    sent(u_all.at[pl.ds(0, (OUT * TEN - 1) * rows), :], 2)
    sent(g_send, 3)
    sent(g_send, 4)
    sent(att_recv, 5)

    def close(c):
        slope = gelu_slope(pre[:, cols(c)].astype(jnp.float32))

        @pl.when(o == 0)
        def _():
            landed(items(1), z_r.at[steps + c])
            hid_out[:, cols(c)] = (
                hid_out[:, cols(c)] + h_left[c, o].astype(jnp.float32)) * slope

        @pl.when(o == OUT - 1)
        def _():
            landed(items(1), z_r.at[steps + c])
            hid_out[:, cols(c)] = (
                hid_out[:, cols(c)] + h_right[c, o].astype(jnp.float32)) * slope

        @pl.when((o > 0) & (o < OUT - 1))
        def _():
            landed(items(2), z_r.at[steps + c])
            hid_out[:, cols(c)] = (
                hid_out[:, cols(c)] + h_right[c, o].astype(jnp.float32)
                + h_left[c, o].astype(jnp.float32)) * slope

    loop(CHUNKS, close)

    @pl.when(o < OUT - 1)
    def _():
        sent(a_all, 0)

    @pl.when(o > 0)
    def _():
        sent(a_all, 1)


def write_out(att, hid, wg, att_hbm, hid_hbm, wg_hbm, sem):
    pairs = ((att, att_hbm), (hid, hid_hbm), (wg, wg_hbm))
    for n, (src, dst) in enumerate(pairs):
        step = src.shape[0] // PIECES
        for p in range(PIECES):
            span = pl.ds(p * step, step)
            pltpu.make_async_copy(src.at[span, :], dst.at[span, :], sem.at[n]).start()
    for n, (src, dst) in enumerate(pairs):
        pltpu.make_async_copy(src, dst, sem.at[n]).wait()


def body(sizes, qkv, segment_ids, out_weight, out_bias, upstream, pre_act, down_weight):
    OUT, INN, TEN = sizes
    rows, width = upstream.shape
    tokens, ff = pre_act.shape
    rows_w = down_weight.shape[0]
    fc = ff // CHUNKS
    bf, f32 = jnp.bfloat16, jnp.float32
    vmem = pl.BlockSpec(memory_space=pltpu.VMEM)
    anym = pl.BlockSpec(memory_space=pl.ANY)
    dma = lambda *shape: pltpu.SemaphoreType.DMA(shape)
    block = min(tokens, 4 * ROWS_DEV)
    held = 4 * (rows * width + tokens * ff + rows_w * ff)
    attention_out, act_grad, weight_grad = pl.pallas_call(
        functools.partial(kernel, sizes),
        out_shape=(
            pltpu.VMEM((rows, width), f32),
            pltpu.VMEM((tokens, ff), f32),
            pltpu.VMEM((rows_w, ff), f32),
        ),
        in_specs=[anym] * 7,
        out_specs=(vmem, vmem, vmem),
        scratch_shapes=[
            pltpu.VMEM(segment_ids.shape, segment_ids.dtype),
            pltpu.VMEM(out_bias.shape, bf),
            pltpu.VMEM(qkv.shape, bf),
            pltpu.VMEM(out_weight.shape, bf),
            pltpu.VMEM((tokens, qkv.shape[2]), bf),
            pltpu.VMEM((tokens, width), bf),
            pltpu.VMEM((TEN - 1, rows, width), bf),
            pltpu.VMEM((rows, width), bf),
            pltpu.VMEM((OUT * tokens, INN * rows_w), bf),
            pltpu.VMEM((INN * rows_w, OUT * tokens), bf),
            pltpu.VMEM((CHUNKS, INN * rows_w, fc), bf),
            pltpu.VMEM((CHUNKS, OUT * tokens, fc), bf),
            pltpu.VMEM((tokens, ff), bf),
            pltpu.VMEM((tokens // block, block, block), f32),
            pltpu.VMEM((CHUNKS, OUT, tokens, fc), bf),
            pltpu.VMEM((CHUNKS, OUT, tokens, fc), bf),
            pltpu.VMEM((CHUNKS, INN - 1, rows_w, fc), bf),
            pltpu.VMEM((CHUNKS, INN - 1, rows_w, fc), bf),
            dma(7), dma(6), dma((OUT + 1) * CHUNKS), dma(OUT - 1), dma(CHUNKS), dma(4),
            pltpu.SemaphoreType.REGULAR((2,)),
        ],
        compiler_params=pltpu.CompilerParams(
            has_side_effects=True, collective_id=0, vmem_limit_bytes=64_000_000 - held),
        name="layer",
    )(qkv, segment_ids, out_weight, out_bias, upstream, pre_act, down_weight)
    results = tuple(
        pltpu.with_memory_space_constraint(r, pltpu.VMEM)
        for r in (attention_out, act_grad, weight_grad))
    return pl.pallas_call(
        write_out,
        out_shape=tuple(jax.ShapeDtypeStruct(r.shape, f32) for r in results),
        in_specs=[vmem] * 3,
        out_specs=(anym,) * 3,
        scratch_shapes=[dma(3)],
        compiler_params=pltpu.CompilerParams(vmem_limit_bytes=2**20),
        name="write_out",
    )(*results)


def solution(mesh):
    dp, tensor = mesh.shape["dp"], mesh.shape["tensor"]
    inner = 2 ** ((dp.bit_length() - 1) // 2)
    return jax.shard_map(
        functools.partial(body, (dp // inner, inner, tensor)),
        mesh=mesh,
        in_specs=(
            P(None, "dp", "tensor"),
            P("dp", None, None),
            P(None, "tensor"),
            P(),
            P(("dp", "tensor"), None),
            P("dp", "tensor"),
            P("dp", "tensor"),
        ),
        out_specs=(P(("dp", "tensor"), None), P("dp", "tensor"), P("dp", "tensor")),
        check_vma=False,
    )
```

```python
import functools
import math

import jax
import jax.numpy as jnp
from jax import lax
from jax.experimental import pallas as pl
from jax.experimental.pallas import tpu as pltpu
from jax.sharding import PartitionSpec as P

HEAD = 128
ROWS_DEV = 64
CHUNKS = 4
GROUP = 2
DELAY = 1
PIECES = 4

root_half = 1.0 / math.sqrt(2.0)
inv_root_tau = 1.0 / math.sqrt(2.0 * math.pi)


def gelu_exact(argument):
    return 0.5 * argument * (1.0 + lax.erf(argument * root_half))


def gelu_slope(argument):
    return (
        0.5 * (1.0 + lax.erf(argument * root_half))
        + argument * jnp.exp(-0.5 * argument * argument) * inv_root_tau
    )


def kernel(
    sizes,
    qkv_hbm, names_hbm, ow_hbm, bias_hbm, up_hbm, pre_hbm, w_hbm,
    att_out, hid_out, wg_out,
    segments, bias, qkv, ow, ctx, part, att_recv,
    up, u_all, u_t, w_all, a_all, pre, same_ref, h_right, h_left, g_send, g_recv,
    local_sem, send_sem, z_r, uz_r, w_r, all_r, far_sem,
):
    OUT, INN, TEN = sizes
    XS = TEN // 2
    g = lax.axis_index("dp")
    t = lax.axis_index("tensor")
    o, i = g // INN, lax.rem(g, INN)
    x, core = t // 2, lax.rem(t, 2)
    rows_w, ff = w_hbm.shape
    rows = up_hbm.shape[0]
    tokens = rows * TEN
    fc = ff // CHUNKS
    dcols = rows_w * INN
    HOPS = OUT - 1

    def remote(src, dst, ssem, rsem, dp, tensor):
        return pltpu.make_async_remote_copy(
            src_ref=src, dst_ref=dst, send_sem=ssem, recv_sem=rsem,
            device_id={"dp": dp, "tensor": tensor},
            device_id_type=pl.DeviceIdType.MESH,
        )

    def cols(c):
        return pl.ds(pl.multiple_of(c * fc, fc), fc)

    def u_rows(oo, tt):
        return u_all.at[pl.ds(pl.multiple_of((oo * TEN + tt) * rows, rows), rows), :]

    def a_rows(c, oo):
        return a_all.at[c, pl.ds(pl.multiple_of(oo * tokens, tokens), tokens), :]

    def w_rows(c, ii):
        return w_all.at[c, pl.ds(pl.multiple_of(ii * rows_w, rows_w), rows_w), :]

    def uz(j):
        to = lax.rem(o + j, OUT)
        return remote(
            up.at[:, pl.ds(pl.multiple_of(to * dcols, dcols), dcols)],
            u_rows(o, t), send_sem.at[2], uz_r.at[j - 1], to * INN + i, t,
        )

    def ux(j, k):
        block = u_rows(lax.rem(o - j + OUT, OUT), t)
        return remote(block, block, send_sem.at[2], all_r.at[0], g,
                      lax.rem(x + k, XS) * 2 + core)

    def uc(j, k):
        block = u_rows(lax.rem(o - j + OUT, OUT), lax.rem(x - k + XS, XS) * 2 + core)
        return remote(block, block, send_sem.at[2], all_r.at[1], g, x * 2 + 1 - core)

    def wx(c, j):
        return remote(w_hbm.at[:, cols(c)], w_rows(c, i), send_sem.at[3], w_r.at[c],
                      o * INN + lax.rem(i + j, INN), t)

    def a_right(c, s, n):
        block = a_rows(c, jnp.maximum(o - s, 0))
        return remote(block, block, send_sem.at[0], z_r.at[n],
                      jnp.minimum(o + 1, OUT - 1) * INN + i, t)

    def a_left(c, s, n):
        block = a_rows(c, jnp.minimum(o + s, OUT - 1))
        return remote(block, block, send_sem.at[1], z_r.at[n],
                      jnp.maximum(o - 1, 0) * INN + i, t)

    def h_r(c, e, n):
        return remote(h_right.at[c, e], h_right.at[c, e], send_sem.at[0], z_r.at[n],
                      jnp.minimum(o + 1, OUT - 1) * INN + i, t)

    def h_l(c, e, n):
        return remote(h_left.at[c, e], h_left.at[c, e], send_sem.at[1], z_r.at[n],
                      jnp.maximum(o - 1, 0) * INN + i, t)

    def gx(c, j):
        return remote(g_send.at[c, j - 1], g_recv.at[c, j - 1], send_sem.at[4], all_r.at[3],
                      o * INN + lax.rem(i + j, INN), t)

    def att(j):
        to = lax.rem(t + j, TEN)
        return remote(part.at[pl.ds(pl.multiple_of(to * rows, rows), rows), :],
                      att_recv.at[j - 1], send_sem.at[5], all_r.at[2], g, to)

    def own_w(c):
        return pltpu.make_async_copy(w_hbm.at[:, cols(c)], w_rows(c, i), local_sem.at[6])

    def sent(ref, stream):
        remote(ref, ref, send_sem.at[stream], send_sem.at[stream], g, t).wait_send()

    def landed(ref, semaphore):
        remote(ref, ref, semaphore, semaphore, g, t).wait_recv()

    def loop(count, fn):
        def step(index, carry):
            fn(index)
            return carry
        lax.fori_loop(0, count, step, 0)

    load_up = pltpu.make_async_copy(up_hbm, up, local_sem.at[0])
    near = sorted({1, OUT - 1})
    far = list(range(2, OUT - 1))
    load_qkv = pltpu.make_async_copy(qkv_hbm, qkv, local_sem.at[1])
    load_ow = pltpu.make_async_copy(ow_hbm, ow, local_sem.at[2])
    load_pre = pltpu.make_async_copy(pre_hbm, pre, local_sem.at[3])

    load_names = pltpu.make_async_copy(names_hbm, segments, local_sem.at[4])
    load_bias = pltpu.make_async_copy(bias_hbm, bias, local_sem.at[5])

    def signal(semaphore, dp, tensor):
        pl.semaphore_signal(semaphore, inc=1, device_id={"dp": dp, "tensor": tensor},
                            device_id_type=pl.DeviceIdType.MESH)

    partners = (
        [(o * INN + lax.rem(i + j, INN), t) for j in range(1, INN)]
        + [(g, lax.rem(t + j, TEN)) for j in range(1, TEN)])
    barrier = pltpu.get_barrier_semaphore()

    @pl.when(o < OUT - 1)
    def _():
        signal(barrier, jnp.minimum(o + 1, OUT - 1) * INN + i, t)

    @pl.when(o > 0)
    def _():
        signal(barrier, jnp.maximum(o - 1, 0) * INN + i, t)

    for dp, tensor in partners:
        signal(barrier, dp, tensor)
    load_up.start()
    load_pre.start()
    load_up.wait()
    sides = jnp.minimum(o, 1) + jnp.minimum(OUT - 1 - o, 1)
    pl.semaphore_wait(barrier, len(partners) + sides)

    def uz_near(to):
        return (to - o == 1) | (o - to == 1)

    for j in near:
        @pl.when(uz_near(lax.rem(o + j, OUT)))
        def _():
            uz(j).start()
    def start_w(c):
        for j in range(1, INN):
            wx(c, j).start()
        own_w(c).start()

    if OUT > 2:
        @pl.when(o >= 2)
        def _():
            pl.semaphore_wait(far_sem.at[0], 1)

        @pl.when((o >= 1) & (o <= OUT - 2))
        def _():
            signal(far_sem.at[0], jnp.minimum(o + 1, OUT - 1) * INN + i, t)

        loop(CHUNKS, start_w)

        @pl.when(o <= OUT - 3)
        def _():
            pl.semaphore_wait(far_sem.at[1], 1)

        @pl.when((o >= 1) & (o <= OUT - 2))
        def _():
            signal(far_sem.at[1], jnp.maximum(o - 1, 0) * INN + i, t)
    else:
        loop(CHUNKS, start_w)
    for j in range(1, OUT):
        @pl.when(jnp.logical_not(uz_near(lax.rem(o + j, OUT))))
        def _():
            uz(j).start()
    load_names.start()
    load_bias.start()
    load_qkv.start()
    load_ow.start()
    u_all[pl.ds(pl.multiple_of((o * TEN + t) * rows, rows), rows), :] = (
        up[:, pl.ds(pl.multiple_of(o * dcols, dcols), dcols)])

    right = (o, lambda p: p, a_right, h_right, h_r)
    left = (OUT - 1 - o, lambda p: OUT - 1 - p, a_left, h_left, h_l)
    steps = OUT * CHUNKS

    def items(count):
        return a_all.at[0, pl.ds(0, count * tokens), :]

    def relayed(n):
        used = 0
        for r in (o, OUT - 1 - o):
            own = (n < (r + 1) * CHUNKS) & (lax.rem(n, (r + 1) * GROUP) < GROUP)
            used = used + jnp.where((r > 0) & (r < OUT - 1) & jnp.logical_not(own), 1, 0)
        for count in (1, 2):
            @pl.when(used == count)
            def _():
                landed(items(count), z_r.at[n])

    def a_item(direction, n):
        r, _, copy, _, _ = direction
        turn = (r + 1) * GROUP
        rest = lax.rem(n, turn)
        s = rest // GROUP
        c = n // turn * GROUP + lax.rem(rest, GROUP)

        @pl.when((r < OUT - 1) & (n < (r + 1) * CHUNKS))
        def _():
            later = n + (n // turn + 1) * GROUP
            copy(c, s, jnp.where(r == OUT - 2, c, later)).start()

    def activate(c):
        act = gelu_exact(pre[:, cols(c)].astype(jnp.float32)).astype(jnp.bfloat16)
        a_all[c, pl.ds(pl.multiple_of(o * tokens, tokens), tokens), :] = act

    def open_group(n):
        activate(n)
        a_item(right, n)
        a_item(left, n)

    load_pre.wait()
    loop(GROUP, open_group)
    for k in range(1, XS):
        ux(0, k).start()
    uc(0, 0).start()
    loop(CHUNKS - GROUP, lambda n: activate(n + GROUP))

    heads = qkv.shape[2] // HEAD
    block = min(tokens, 4 * ROWS_DEV)
    scale = 1.0 / math.sqrt(HEAD)

    load_names.wait()
    load_bias.wait()
    labels = segments[0].astype(jnp.float32)
    packs, length = labels.shape
    spread = (
        lax.rem(lax.broadcasted_iota(jnp.int32, (length, tokens), 1), length)
        == lax.broadcasted_iota(jnp.int32, (length, tokens), 0)
    ).astype(jnp.float32)
    wide = jnp.dot(labels, spread, preferred_element_type=jnp.float32)
    pack = lax.broadcasted_iota(jnp.int32, (packs, tokens), 0)
    here = lax.broadcasted_iota(jnp.int32, (packs, tokens), 1) // length == pack
    name = jnp.sum(
        jnp.where(here, wide + 2.0 * pack.astype(jnp.float32), 0.0), axis=0, keepdims=True)
    for b in range(tokens // block):
        across = jnp.broadcast_to(name[:, b * block : (b + 1) * block], (block, block))
        same_ref[b] = (across == across.T).astype(jnp.float32)

    def head(h):
        lanes = pl.ds(pl.multiple_of(h * HEAD, HEAD), HEAD)
        for b in range(tokens // block):
            mine = slice(b * block, (b + 1) * block)
            same = same_ref[b] > 0.5
            scores = lax.dot_general(
                qkv[0, mine, lanes], qkv[1, mine, lanes], (((1,), (1,)), ((), ())),
                preferred_element_type=jnp.float32) * scale
            masked = jnp.where(same, scores, -1e30)
            top = jnp.max(masked, axis=1, keepdims=True)
            exponent = jnp.where(same, jnp.exp(masked - top), 0.0)
            weights = (exponent / jnp.sum(exponent, axis=1, keepdims=True)).astype(jnp.bfloat16)
            ctx[mine, lanes] = jnp.dot(
                weights, qkv[2, mine, lanes], preferred_element_type=jnp.float32
            ).astype(jnp.bfloat16)

    nb = 512
    spans = ow.shape[0] // nb

    def project(n):
        span = pl.ds(pl.multiple_of(n * nb, nb), nb)
        part[:, span] = lax.dot_general(
            ctx[...], ow[span, :], (((1,), (1,)), ((), ())),
            preferred_element_type=jnp.float32).astype(jnp.bfloat16)

    def flip(e):
        span = pl.ds(pl.multiple_of(e * tokens, tokens), tokens)
        u_t[:, span] = u_all[span, :].T

    def partial(c, e):
        span = pl.ds(pl.multiple_of(e * tokens, tokens), tokens)
        return jnp.dot(u_all[span, :], w_all[c], preferred_element_type=jnp.float32)

    def h_item(direction, n):
        r, place, _, held, copy = direction
        m = n - (r + 1) * CHUNKS
        e = place(OUT - 1 - m // CHUNKS)
        c = lax.rem(m, CHUNKS)
        slot = n + CHUNKS

        @pl.when((m >= 0) & (r == 0))
        def _():
            held[c, e] = partial(c, e).astype(jnp.bfloat16)
            copy(c, e, slot).start()

        @pl.when((m >= 0) & (r > 0) & (r < OUT - 1))
        def _():
            mine = partial(c, e)
            held[c, e] = (mine + held[c, e].astype(jnp.float32)).astype(jnp.bfloat16)
            copy(c, e, slot).start()

    def weight_chunk(c):
        for direction in (right, left):
            @pl.when(direction[0] == OUT - 1)
            def _():
                landed(items(OUT - 1), z_r.at[c])
        for j in range(1, INN):
            to = lax.rem(i + j, INN)
            span = pl.ds(pl.multiple_of(to * rows_w, rows_w), rows_w)
            g_send[c, j - 1] = jnp.dot(
                u_t[span, :], a_all[c], preferred_element_type=jnp.float32).astype(jnp.bfloat16)
            gx(c, j).start()
        span = pl.ds(pl.multiple_of(i * rows_w, rows_w), rows_w)
        wg_out[:, cols(c)] = jnp.dot(
            u_t[span, :], a_all[c], preferred_element_type=jnp.float32)

    load_qkv.wait()
    loop(heads, head)

    for j in range(1, OUT):
        uz(j).wait_recv()
        for k in range(1, XS):
            ux(j, k).start()
        uc(j, 0).start()
    load_ow.wait()
    early = spans // 2
    loop(early, project)

    def relay(n):
        relayed(n)
        a_item(right, n)
        a_item(left, n)

    loop(CHUNKS - GROUP - 1, lambda n: relay(n + GROUP))
    if XS > 1:
        landed(u_all.at[pl.ds(0, OUT * (XS - 1) * rows), :], all_r.at[0])
    for j in range(OUT):
        for k in range(1, XS):
            uc(j, k).start()
    relay(CHUNKS - 1)
    landed(u_all.at[pl.ds(0, OUT * XS * rows), :], all_r.at[1])
    loop(OUT, flip)
    own_rows = g_send.at[:, 0]
    pltpu.make_async_copy(own_rows, own_rows, local_sem.at[6]).wait()
    lead = max(DELAY, CHUNKS - 1 - (OUT - 2) * GROUP) + 1 + (OUT - 2) * GROUP

    def tick(k):
        n = k + CHUNKS
        first = k

        @pl.when(first < CHUNKS)
        def _():
            landed(g_recv.at[first], w_r.at[first])

        relayed(n)
        for direction in (right, left):
            a_item(direction, n)
            h_item(direction, n)

        @pl.when(first < CHUNKS)
        def _():
            hid_out[:, cols(first)] = partial(first, o)

        @pl.when(k < spans - early)
        def _():
            project(k + early)

        @pl.when(k == spans - early)
        def _():
            for j in range(1, TEN):
                att(j).start()

        m = n - lead
        turn = (OUT - 1) * GROUP
        rest = lax.rem(m, turn)

        @pl.when((m >= 0) & (rest < GROUP) & (m // turn * GROUP < CHUNKS))
        def _():
            weight_chunk(m // turn * GROUP + rest)

    loop((OUT - 1) * CHUNKS, tick)

    total = part[pl.ds(pl.multiple_of(t * rows, rows), rows), :].astype(jnp.float32)
    total = total + bias[...].astype(jnp.float32)[None, :]
    landed(att_recv, all_r.at[2])
    for j in range(1, TEN):
        total = total + att_recv[j - 1].astype(jnp.float32)
    att_out[...] = total

    factor = 1.0 / (OUT * INN)

    landed(g_recv, all_r.at[3])

    def finish(c):
        acc = wg_out[:, cols(c)]
        for j in range(1, INN):
            acc = acc + g_recv[c, j - 1].astype(jnp.float32)
        wg_out[:, cols(c)] = acc * factor

    loop(CHUNKS, finish)
    sent(u_all.at[pl.ds(0, (OUT * TEN - 1) * rows), :], 2)
    sent(g_send, 3)
    sent(g_send, 4)
    sent(att_recv, 5)

    def close(c):
        slope = gelu_slope(pre[:, cols(c)].astype(jnp.float32))

        @pl.when(o == 0)
        def _():
            landed(items(1), z_r.at[steps + c])
            hid_out[:, cols(c)] = (
                hid_out[:, cols(c)] + h_left[c, o].astype(jnp.float32)) * slope

        @pl.when(o == OUT - 1)
        def _():
            landed(items(1), z_r.at[steps + c])
            hid_out[:, cols(c)] = (
                hid_out[:, cols(c)] + h_right[c, o].astype(jnp.float32)) * slope

        @pl.when((o > 0) & (o < OUT - 1))
        def _():
            landed(items(2), z_r.at[steps + c])
            hid_out[:, cols(c)] = (
                hid_out[:, cols(c)] + h_right[c, o].astype(jnp.float32)
                + h_left[c, o].astype(jnp.float32)) * slope

    loop(CHUNKS, close)

    @pl.when(o < OUT - 1)
    def _():
        sent(a_all, 0)

    @pl.when(o > 0)
    def _():
        sent(a_all, 1)


def write_out(att, hid, wg, att_hbm, hid_hbm, wg_hbm, sem):
    pairs = ((att, att_hbm), (hid, hid_hbm), (wg, wg_hbm))
    for n, (src, dst) in enumerate(pairs):
        step = src.shape[0] // PIECES
        for p in range(PIECES):
            span = pl.ds(p * step, step)
            pltpu.make_async_copy(src.at[span, :], dst.at[span, :], sem.at[n]).start()
    for n, (src, dst) in enumerate(pairs):
        pltpu.make_async_copy(src, dst, sem.at[n]).wait()


def body(sizes, qkv, segment_ids, out_weight, out_bias, upstream, pre_act, down_weight):
    OUT, INN, TEN = sizes
    rows, width = upstream.shape
    tokens, ff = pre_act.shape
    rows_w = down_weight.shape[0]
    fc = ff // CHUNKS
    bf, f32 = jnp.bfloat16, jnp.float32
    vmem = pl.BlockSpec(memory_space=pltpu.VMEM)
    anym = pl.BlockSpec(memory_space=pl.ANY)
    dma = lambda *shape: pltpu.SemaphoreType.DMA(shape)
    block = min(tokens, 4 * ROWS_DEV)
    held = 4 * (rows * width + tokens * ff + rows_w * ff)
    attention_out, act_grad, weight_grad = pl.pallas_call(
        functools.partial(kernel, sizes),
        out_shape=(
            pltpu.VMEM((rows, width), f32),
            pltpu.VMEM((tokens, ff), f32),
            pltpu.VMEM((rows_w, ff), f32),
        ),
        in_specs=[anym] * 7,
        out_specs=(vmem, vmem, vmem),
        scratch_shapes=[
            pltpu.VMEM(segment_ids.shape, segment_ids.dtype),
            pltpu.VMEM(out_bias.shape, bf),
            pltpu.VMEM(qkv.shape, bf),
            pltpu.VMEM(out_weight.shape, bf),
            pltpu.VMEM((tokens, qkv.shape[2]), bf),
            pltpu.VMEM((tokens, width), bf),
            pltpu.VMEM((TEN - 1, rows, width), bf),
            pltpu.VMEM((rows, width), bf),
            pltpu.VMEM((OUT * tokens, INN * rows_w), bf),
            pltpu.VMEM((INN * rows_w, OUT * tokens), bf),
            pltpu.VMEM((CHUNKS, INN * rows_w, fc), bf),
            pltpu.VMEM((CHUNKS, OUT * tokens, fc), bf),
            pltpu.VMEM((tokens, ff), bf),
            pltpu.VMEM((tokens // block, block, block), f32),
            pltpu.VMEM((CHUNKS, OUT, tokens, fc), bf),
            pltpu.VMEM((CHUNKS, OUT, tokens, fc), bf),
            pltpu.VMEM((CHUNKS, INN - 1, rows_w, fc), bf),
            pltpu.VMEM((CHUNKS, INN - 1, rows_w, fc), bf),
            dma(7), dma(6), dma((OUT + 1) * CHUNKS), dma(OUT - 1), dma(CHUNKS), dma(4),
            pltpu.SemaphoreType.REGULAR((2,)),
        ],
        compiler_params=pltpu.CompilerParams(
            has_side_effects=True, collective_id=0, vmem_limit_bytes=64_000_000 - held),
        name="layer",
    )(qkv, segment_ids, out_weight, out_bias, upstream, pre_act, down_weight)
    results = tuple(
        pltpu.with_memory_space_constraint(r, pltpu.VMEM)
        for r in (attention_out, act_grad, weight_grad))
    return pl.pallas_call(
        write_out,
        out_shape=tuple(jax.ShapeDtypeStruct(r.shape, f32) for r in results),
        in_specs=[vmem] * 3,
        out_specs=(anym,) * 3,
        scratch_shapes=[dma(3)],
        compiler_params=pltpu.CompilerParams(vmem_limit_bytes=2**20),
        name="write_out",
    )(*results)


def solution(mesh):
    dp, tensor = mesh.shape["dp"], mesh.shape["tensor"]
    inner = 2 ** ((dp.bit_length() - 1) // 2)
    return jax.shard_map(
        functools.partial(body, (dp // inner, inner, tensor)),
        mesh=mesh,
        in_specs=(
            P(None, "dp", "tensor"),
            P("dp", None, None),
            P(None, "tensor"),
            P(),
            P(("dp", "tensor"), None),
            P("dp", "tensor"),
            P("dp", "tensor"),
        ),
        out_specs=(P(("dp", "tensor"), None), P("dp", "tensor"), P("dp", "tensor")),
        check_vma=False,
    )
```
